32 devices in a mesh: dp: 1 (over z), sx: 4 (over y), sy: 8 (over x, core).
Axes of the slice: x: 4, y: 4, z: 1, core: 2. Of those that a mesh axis runs over, the one named last changes fastest.
The devices are a block of a 4x4x8 slice.
Arguments:
- act_in: bfloat16 [2, 2048, 32, 256], P('dp', 'sy', 'sx')
- norm_first: bfloat16 [2, 256], replicated
- w_first: bfloat16 [3, 3, 256, 128], replicated
- w_short: bfloat16 [256, 128], replicated
- norm_rest: bfloat16 [6, 2, 128], replicated
- w_rest: bfloat16 [5, 3, 3, 128, 128], replicated
- bias_rest: bfloat16 [7, 128], replicated
- w_out: bfloat16 [3, 3, 128, 3], replicated
- bias_out: bfloat16 [3], replicated
Outputs:
- output: float32 [2, 2048, 32, 3], P('dp', 'sy', 'sx')
All inputs are finite; a program needn't handle non-finite values.
Results may differ from the reference program's by a relative error of at most 0.00887721.
Values are sent between devices in bfloat16 or wider.
A program may use at most 768 MiB of HBM per device.

```python
import math
import jax
import jax.numpy as jnp
from jax import lax

SAMPLES = 2
IMG_H = 2048
IMG_W = 32
IN_CH = 256
MID_CH = 128
OUT_CH = 3
GROUPS = 32
GN_EPS = 1e-6


def normal_weight(key, shape, fan_in):
    return (jax.random.normal(key, shape, jnp.float32) * fan_in ** -0.5).astype(jnp.bfloat16)


def norm_params(key, layer_count, chan_count):
    gain_key, shift_key = jax.random.split(key)
    gains = 1.0 + 0.25 * jax.random.normal(gain_key, (layer_count, chan_count), jnp.float32)
    shifts = 0.25 * jax.random.normal(shift_key, (layer_count, chan_count), jnp.float32)
    return jnp.stack([gains, shifts], axis=1).astype(jnp.bfloat16)


def setup_inputs(seed: int = 0, part: int = 0) -> dict:
    base_key = jax.random.key(seed)
    act_keys = jax.random.split(jax.random.fold_in(base_key, part), 6)
    weight_keys = jax.random.split(base_key, 8)
    wave_count = 3
    base_noise = jax.random.normal(act_keys[0], (SAMPLES, IMG_H, IMG_W, IN_CH), jnp.float32)
    wave_amp = jax.random.normal(act_keys[1], (SAMPLES, wave_count, 1, IN_CH), jnp.float32)
    row_freq = jax.random.uniform(act_keys[2], (SAMPLES, wave_count, 1, 1), jnp.float32, 0.5, 2.5)
    col_freq = jax.random.uniform(act_keys[3], (SAMPLES, wave_count, 1, 1), jnp.float32, 0.5, 2.5)
    row_phase = jax.random.uniform(act_keys[4], (SAMPLES, wave_count, 1, IN_CH), jnp.float32, 0.0, 2.0 * math.pi)
    col_phase = jax.random.uniform(act_keys[5], (SAMPLES, wave_count, 1, IN_CH), jnp.float32, 0.0, 2.0 * math.pi)
    row_pos = (jnp.arange(IMG_H, dtype=jnp.float32) / IMG_H)[:, None]
    col_pos = (jnp.arange(IMG_W, dtype=jnp.float32) / IMG_W)[:, None]
    row_wave = wave_amp * jnp.cos(2.0 * math.pi * row_freq * row_pos + row_phase)
    col_wave = jnp.cos(2.0 * math.pi * col_freq * col_pos + col_phase)
    smooth_field = jnp.einsum("skhc,skwc->shwc", row_wave, col_wave)
    act_in = (0.7 * base_noise + smooth_field).astype(jnp.bfloat16)
    return {
        "act_in": act_in,
        "norm_first": norm_params(weight_keys[0], 1, IN_CH)[0],
        "w_first": normal_weight(weight_keys[1], (3, 3, IN_CH, MID_CH), 9 * IN_CH),
        "w_short": normal_weight(weight_keys[2], (IN_CH, MID_CH), IN_CH),
        "norm_rest": norm_params(weight_keys[3], 6, MID_CH),
        "w_rest": normal_weight(weight_keys[4], (5, 3, 3, MID_CH, MID_CH), 9 * MID_CH),
        "bias_rest": (0.3 * jax.random.normal(weight_keys[5], (7, MID_CH), jnp.float32)).astype(jnp.bfloat16),
        "w_out": normal_weight(weight_keys[6], (3, 3, MID_CH, OUT_CH), 9 * MID_CH),
        "bias_out": (0.3 * jax.random.normal(weight_keys[7], (OUT_CH,), jnp.float32)).astype(jnp.bfloat16),
    }


def group_norm_act(act_map, norm_pair):
    num_rows, num_cols, channels = act_map.shape
    per_group = channels // GROUPS
    group_count = num_rows * num_cols * per_group
    sum_one = jnp.sum(act_map, axis=(0, 1), dtype=jnp.float32).reshape(GROUPS, per_group).sum(axis=1)
    sum_two = jnp.sum(jnp.square(act_map.astype(jnp.float32)), axis=(0, 1)).reshape(GROUPS, per_group).sum(axis=1)
    group_mean = sum_one / group_count
    inv_std = lax.rsqrt(sum_two / group_count - group_mean * group_mean + GN_EPS)
    chan_scale = jnp.repeat(inv_std, per_group) * norm_pair[0].astype(jnp.float32)
    chan_shift = norm_pair[1].astype(jnp.float32) - jnp.repeat(group_mean, per_group) * chan_scale
    return jax.nn.silu(act_map.astype(jnp.float32) * chan_scale + chan_shift).astype(jnp.bfloat16)


def conv_three(act_map, kernel):
    num_rows, num_cols, in_chans = act_map.shape
    padded = jnp.pad(act_map, ((1, 1), (1, 1), (0, 0)))
    accum_sum = jnp.zeros((num_rows * num_cols, kernel.shape[3]), jnp.float32)
    for row_off in range(3):
        for col_off in range(3):
            window = padded[row_off:row_off + num_rows, col_off:col_off + num_cols].reshape(num_rows * num_cols, in_chans)
            accum_sum = accum_sum + jnp.dot(window, kernel[row_off, col_off], preferred_element_type=jnp.float32)
    return accum_sum.reshape(num_rows, num_cols, kernel.shape[3])


def reference(act_in, norm_first, w_first, w_short, norm_rest, w_rest, bias_rest, w_out, bias_out):
    bias_rows = bias_rest.astype(jnp.float32)

    def decode_sample(sample):
        num_rows, num_cols, in_chans = sample.shape
        mid_act = (conv_three(group_norm_act(sample, norm_first), w_first) + bias_rows[0]).astype(jnp.bfloat16)
        skip_path = jnp.dot(sample.reshape(num_rows * num_cols, in_chans), w_short, preferred_element_type=jnp.float32).reshape(num_rows, num_cols, -1) + bias_rows[6]
        hidden = (conv_three(group_norm_act(mid_act, norm_rest[0]), w_rest[0]) + bias_rows[1] + skip_path).astype(jnp.bfloat16)
        for res_index in range(1, 3):
            first_at = 2 * res_index - 1
            mid_act = (conv_three(group_norm_act(hidden, norm_rest[first_at]), w_rest[first_at]) + bias_rows[first_at + 1]).astype(jnp.bfloat16)
            hidden = (conv_three(group_norm_act(mid_act, norm_rest[first_at + 1]), w_rest[first_at + 1]) + bias_rows[first_at + 2] + hidden.astype(jnp.float32)).astype(jnp.bfloat16)
        return conv_three(group_norm_act(hidden, norm_rest[5]), w_out) + bias_out.astype(jnp.float32)

    return lax.map(decode_sample, act_in)
```

```python
import functools

import jax
import jax.numpy as jnp
from jax import lax
from jax.experimental import pallas as pl
from jax.experimental.pallas import tpu as pltpu
from jax.sharding import PartitionSpec as P

GROUPS = 32
GN_EPS = 1e-6
LANES = 128
MESH = pl.DeviceIdType.MESH
F32 = jnp.float32
BF16 = jnp.bfloat16


def half_silu(half):
    return half + half * jnp.tanh(half)


def decode_kernel(rows_n, cols_n, act_hbm, w_first_hbm, w_short_hbm, w_rest_hbm, norm_first_ref, norm_rest_ref, bias_ref, w_out_ref, out_ref,
                  raw, flat, map_in, maps, sh, z_in, z_mid, short, w_first, w_short, w_rest, w_head, ones_in, ones_mid,
                  msg_in, msg_mid, got_in, got_mid, edge_in, edge_mid, halo_in, halo_mid,
                  act_sem, weight_sem, stat_recv, stat_send, halo_recv, halo_send):
    samples, rows, cols, in_ch = raw.shape
    halves = in_ch // LANES
    layers = w_rest.shape[0] + 1
    peers_n = rows_n * cols_n - 1
    sx = lax.axis_index("sx")
    sy = lax.axis_index("sy")
    core = lax.rem(sy, 2)
    chip = sy // 2
    chips_n = rows_n // 2

    def ring(offset, size):
        return min(offset, size - offset)

    offsets = [(dx, dy, dc) for dx in range(cols_n) for dy in range(chips_n) for dc in range(2) if (dx, dy, dc) != (0, 0, 0)]
    offsets.sort(key=lambda o: (-ring(o[0], cols_n) - ring(o[1], chips_n), -o[2]))

    def peer(offset):
        dx, dy, dc = offset
        return {"sx": lax.rem(sx + dx, cols_n), "sy": lax.rem(chip + dy, chips_n) * 2 + lax.rem(core + dc, 2)}

    for s in range(samples):
        pltpu.make_async_copy(act_hbm.at[s], raw.at[s], act_sem.at[s]).start()
    for o in range(2):
        for dc in range(3):
            pltpu.make_async_copy(w_first_hbm.at[:, dc], w_first.at[o + dc, :, :, pl.ds(o * LANES, LANES)], weight_sem.at[0]).start()
    pltpu.make_async_copy(w_short_hbm, w_short, weight_sem.at[layers]).start()
    for k in range(layers - 1):
        for o in range(2):
            for dc in range(3):
                pltpu.make_async_copy(w_rest_hbm.at[k, :, dc], w_rest.at[k, o + dc, :, :, pl.ds(o * LANES, LANES)], weight_sem.at[k + 1]).start()

    barrier = pltpu.get_barrier_semaphore()
    for offset in offsets:
        pl.semaphore_signal(barrier, inc=1, device_id=peer(offset), device_id_type=MESH)

    row_id = lax.broadcasted_iota(jnp.int32, (LANES, LANES), 0)
    lane_id = lax.broadcasted_iota(jnp.int32, (LANES, LANES), 1)
    for ones, per_group in ((ones_in, in_ch // GROUPS), (ones_mid, LANES // GROUPS)):
        ones[...] = jnp.where(row_id // per_group == lane_id // per_group, 1.0, 0.0).astype(F32)
    for dr in range(3):
        w_first[3, dr, :, 0:LANES] = jnp.zeros((in_ch, LANES), BF16)
        w_first[0, dr, :, LANES:] = jnp.zeros((in_ch, LANES), BF16)

        def clear(k, _):
            w_rest[k, 3, dr, :, 0:LANES] = jnp.zeros((LANES, LANES), BF16)
            w_rest[k, 0, dr, :, LANES:] = jnp.zeros((LANES, LANES), BF16)
            return 0

        lax.fori_loop(0, layers - 1, clear, 0)

    @pl.when(sx == 0)
    def _():
        z_in[:, 0:3 * in_ch] = jnp.zeros((rows, 3 * in_ch), BF16)
        z_mid[:, 0:3 * LANES] = jnp.zeros((rows, 3 * LANES), BF16)

    @pl.when(sx == cols_n - 1)
    def _():
        z_in[:, (cols + 1) * 3 * in_ch:] = jnp.zeros((rows, 3 * in_ch), BF16)
        z_mid[:, (cols + 1) * 3 * LANES:] = jnp.zeros((rows, 3 * LANES), BF16)

    has = {"up": sy > 0, "down": sy < rows_n - 1, "left": sx > 0, "right": sx < cols_n - 1}

    def both(one, two):
        return jnp.logical_and(has[one], has[two])

    row_moves = [
        (1, 1, 0, {"sy": sy - 1}, has["up"], has["down"]),
        (0, 1, 1, {"sy": sy + 1}, has["down"], has["up"]),
        (1, 2, 0, {"sx": sx - 1, "sy": sy - 1}, both("up", "left"), both("down", "right")),
        (1, 0, 0, {"sx": sx + 1, "sy": sy - 1}, both("up", "right"), both("down", "left")),
        (0, 2, 1, {"sx": sx - 1, "sy": sy + 1}, both("down", "left"), both("up", "right")),
        (0, 0, 1, {"sx": sx + 1, "sy": sy + 1}, both("down", "right"), both("up", "left")),
    ]

    def tile(k, s, c):
        return map_in.at[s, c] if k == 0 else maps.at[k - 1, s, c]

    def edges(k, s):
        return edge_in.at[s] if k == 0 else edge_mid.at[k - 1, s]

    def halo(k, s):
        return halo_in.at[s] if k == 0 else halo_mid.at[k - 1, s]

    def message(k, s):
        return msg_in.at[s] if k == 0 else msg_mid.at[k - 1, s]

    def received(k, s):
        return got_in.at[s] if k == 0 else got_mid.at[k - 1, s]

    def col_copy(k, s, at):
        src, dst, to = ((1, cols + 1, {"sx": sx - 1}), (cols, 0, {"sx": sx + 1}))[at]
        return pltpu.make_async_remote_copy(tile(k, s, src), tile(k, s, dst), halo_send.at[k, s, at], halo_recv.at[k, s, at], device_id=to, device_id_type=MESH)

    def row_copy(k, s, at):
        side, place, edge, to, _, _ = row_moves[at]
        return pltpu.make_async_remote_copy(edges(k, s).at[edge], halo(k, s).at[side, place], halo_send.at[k, s, 2 + at], halo_recv.at[k, s, 2 + at], device_id=to, device_id_type=MESH)

    def send_cols(k, s):
        for at, there in enumerate((has["left"], has["right"])):
            pl.when(there)(lambda at=at: col_copy(k, s, at).start())

    def send_rows(k, s):
        for at, move in enumerate(row_moves):
            pl.when(move[4])(lambda at=at: row_copy(k, s, at).start())

    def send_stats(k, s):
        for slot, offset in enumerate(offsets):
            pltpu.make_async_remote_copy(message(k, s), received(k, s).at[slot], stat_send.at[k, s], stat_recv.at[k, s], device_id=peer(offset), device_id_type=MESH).start()

    def wait_rows(k, s):
        for at, move in enumerate(row_moves):
            pl.when(move[5])(lambda at=at: row_copy(k, s, at).wait_recv())

    def store_stats(k, s, sums):
        target = message(k, s)
        for at, part in enumerate(sums):
            target[at:at + 1, :] = jnp.sum(part, axis=0, keepdims=True)

    def scales(k, s):
        pltpu.make_async_copy(received(k, s), received(k, s), stat_recv.at[k, s]).wait()
        total = message(k, s)[...] + jnp.sum(received(k, s)[...], axis=0)
        ones = ones_in if k == 0 else ones_mid
        total = jnp.dot(total, ones[...], precision=lax.Precision.HIGHEST, preferred_element_type=F32)
        parts = halves if k == 0 else 1
        per_group = parts * LANES // GROUPS
        count = rows * rows_n * cols * cols_n * per_group
        rows_out = []
        for part in range(parts):
            norm = (norm_first_ref[:, part * LANES:(part + 1) * LANES] if k == 0 else norm_rest_ref[k - 1]).astype(F32)
            mean = total[part:part + 1] / count
            square = total[parts + part:parts + part + 1] / count
            scale = lax.rsqrt(square - mean * mean + GN_EPS) * norm[0:1]
            shift = norm[1:2] - mean * scale
            rows_out.append((0.5 * scale, 0.5 * shift))
        return rows_out

    def activate(k, s):
        z = z_in if k == 0 else z_mid
        parts = halves if k == 0 else 1
        scale_rows = scales(k, s)
        wait_rows(k, s)
        for part, (scale, shift) in enumerate(scale_rows):
            for side, there in ((0, "up"), (1, "down")):
                at_row = 7 if side == 0 else 8 + rows
                for place in range(3):
                    source = halo(k, s)[side, place, part]
                    seen = has[there] if place == 1 else both(there, "left" if place == 0 else "right")
                    act = jnp.where(seen, half_silu(source * scale + shift), 0.0)
                    for c in ((0,), range(1, cols + 1), (cols + 1,))[place]:
                        pick = (c + cols - 1) % cols
                        sh[part, c, at_row:at_row + 1, :] = act[pick:pick + 1]

        def column(c):
            for part, (scale, shift) in enumerate(scale_rows):
                ref = map_in.at[s, c, part] if k == 0 else maps.at[k - 1, s, c]
                act = half_silu(ref[...].astype(F32) * scale + shift)
                sh[part, c, 8:8 + rows, :] = act
                for dr in range(3):
                    at = c * 3 * parts * LANES + (dr * parts + part) * LANES
                    z[:, pl.ds(pl.multiple_of(at, LANES), LANES)] = (act if dr == 1 else sh[part, c, 7 + dr:7 + dr + rows, :]).astype(BF16)

        lax.fori_loop(1, cols + 1, lambda c, _: (column(c), 0)[1], 0)
        for at, (there, c) in enumerate((("right", cols + 1), ("left", 0))):

            @pl.when(has[there])
            def _(at=at, c=c):
                col_copy(k, s, at).wait_recv()
                column(c)

    def convolve(k, s):
        z = z_in if k == 0 else z_mid
        depth = 3 * (halves if k == 0 else 1) * LANES
        weights = (w_first[...] if k == 0 else w_rest[k - 1]).reshape(4 * depth, 2 * LANES)
        bias = bias_ref[k:k + 1].astype(F32)
        edge = edges(k + 1, s)

        def pair(p, sums):
            lhs = z[:, pl.ds(pl.multiple_of(p * 2 * depth, LANES), 4 * depth)]
            acc = jnp.dot(lhs, weights, preferred_element_type=F32)
            sum_one, sum_two = sums
            for o in range(2):
                c = 2 * p + o
                value = acc[:, o * LANES:(o + 1) * LANES] + bias
                if k == 1:
                    value = value + short[s, c]
                elif k > 1 and k % 2 == 1:
                    value = value + maps[k - 2, s, c + 1].astype(F32)
                rounded = value.astype(BF16)
                maps[k, s, c + 1] = rounded
                value = rounded.astype(F32)
                edge[0, 0, pl.ds(c, 1), :] = value[0:1]
                edge[1, 0, pl.ds(c, 1), :] = value[rows - 1:rows]
                value = value.reshape(rows // 8, 8, LANES)
                sum_one = sum_one + jnp.sum(value, axis=0)
                sum_two = sum_two + jnp.sum(value * value, axis=0)
            return sum_one, sum_two

        zero = jnp.zeros((8, LANES), F32)
        outer = cols // 2 - 1
        sums = lax.fori_loop(0, 2, lambda i, acc: pair(i * outer, acc), (zero, zero))
        send_cols(k + 1, s)
        sums = lax.fori_loop(1, outer, pair, sums)
        store_stats(k + 1, s, sums)
        send_rows(k + 1, s)
        send_stats(k + 1, s)

    chunk = 16

    def load(s):
        pltpu.make_async_copy(act_hbm.at[s], raw.at[s], act_sem.at[s]).wait()

        def step(i, sums):
            at = pl.multiple_of(i * chunk, chunk)
            sums = list(sums)
            for part in range(halves):
                value = raw[s, pl.ds(at, chunk), :, part * LANES:(part + 1) * LANES].astype(F32)
                flat[s, part, pl.ds(pl.multiple_of(at * cols, chunk * cols), chunk * cols), :] = value.reshape(chunk * cols, LANES)
                sums[part] = sums[part] + jnp.sum(value, axis=0)
                sums[halves + part] = sums[halves + part] + jnp.sum(value * value, axis=0)
            return tuple(sums)

        zero = jnp.zeros((cols, LANES), F32)
        sums = lax.fori_loop(0, rows // chunk, step, (zero,) * (2 * halves))
        store_stats(0, s, sums)
        for part in range(halves):
            edge_in[s, 0, part] = flat[s, part, 0:cols, :]
            edge_in[s, 1, part] = flat[s, part, (rows - 1) * cols:, :]

    def turn(s, c):
        for part in range(halves):
            map_in[s, c + 1, part] = flat[s, part, pl.ds(c, rows, stride=cols), :].astype(BF16)

    for s in range(samples):
        load(s)
        turn(s, 0)
        turn(s, cols - 1)
        if s == 0:
            pl.semaphore_wait(barrier, peers_n)
        send_rows(0, s)
        send_stats(0, s)
        send_cols(0, s)
    for s in range(samples):
        for c in range(1, cols - 1):
            turn(s, c)

    col_id = lax.broadcasted_iota(jnp.int32, (cols, LANES), 0)
    for j in range(cols + 2):
        for dr in range(3):
            blocks = []
            for ch in range(3):
                block = jnp.zeros((cols, LANES), F32)
                for dc in range(3):
                    block = jnp.where(col_id == j - dc, w_out_ref[dr, dc, ch:ch + 1, :].astype(F32), block)
                blocks.append(block)
            blocks.append(jnp.zeros((cols, LANES), F32))
            at = (j * 3 + dr) * LANES
            w_head[:, at:at + LANES] = jnp.concatenate(blocks, axis=0).astype(BF16)

    for k in range(layers):
        if k == 0:
            pltpu.make_async_copy(w_first.at[0:3], w_first.at[0:3], weight_sem.at[0]).wait()
        else:
            pltpu.make_async_copy(w_rest.at[k - 1, 0:3], w_rest.at[k - 1, 0:3], weight_sem.at[k]).wait()
        for s in range(samples):
            activate(k, s)
            convolve(k, s)
        if k == 0:
            pltpu.make_async_copy(w_short_hbm, w_short, weight_sem.at[layers]).wait()
            skip_bias = bias_ref[layers:layers + 1].astype(F32)
            for s in range(samples):

                def skip(c, _):
                    both_halves = jnp.concatenate([map_in[s, c + 1, part] for part in range(halves)], axis=1)
                    short[s, c] = jnp.dot(both_halves, w_short[...], preferred_element_type=F32) + skip_bias
                    return 0

                lax.fori_loop(0, cols, skip, 0)
    for s in range(samples):
        activate(layers, s)
        head = lax.dot_general(w_head[...], z_mid[...], (((1,), (1,)), ((), ())), preferred_element_type=F32)
        for ch in range(3):
            out_ref[s, ch] = head[ch * cols:(ch + 1) * cols]

    for k in range(layers + 1):
        for s in range(samples):
            pltpu.make_async_copy(received(k, s), received(k, s), stat_send.at[k, s]).wait()
            for at, there in enumerate((has["left"], has["right"])):
                pl.when(there)(lambda at=at: col_copy(k, s, at).wait_send())
            for at, move in enumerate(row_moves):
                pl.when(move[4])(lambda at=at: row_copy(k, s, at).wait_send())


def solution(mesh):
    rows_n = mesh.shape["sy"]
    cols_n = mesh.shape["sx"]
    tile_spec = P("dp", "sy", "sx", None)
    replicated = P()

    def local_decode(act_in, norm_first, w_first, w_short, norm_rest, w_rest, bias_rest, w_out, bias_out):
        samples, rows, cols, in_ch = act_in.shape
        halves = in_ch // LANES
        layers = w_rest.shape[0] + 1
        peers_n = rows_n * cols_n - 1
        anywhere = pl.BlockSpec(memory_space=pl.ANY)
        in_vmem = pl.BlockSpec(memory_space=pltpu.VMEM)
        image = pl.pallas_call(
            functools.partial(decode_kernel, rows_n, cols_n),
            out_shape=jax.ShapeDtypeStruct((samples, 3, cols, rows), F32),
            in_specs=[anywhere] * 4 + [in_vmem] * 4,
            out_specs=in_vmem,
            scratch_shapes=[
                pltpu.VMEM((samples, rows, cols, in_ch), BF16),
                pltpu.VMEM((samples, halves, rows * cols, LANES), F32),
                pltpu.VMEM((samples, cols + 2, halves, rows, LANES), BF16),
                pltpu.VMEM((layers, samples, cols + 2, rows, LANES), BF16),
                pltpu.VMEM((halves, cols + 2, rows + 16, LANES), F32),
                pltpu.VMEM((rows, (cols + 2) * 3 * in_ch), BF16),
                pltpu.VMEM((rows, (cols + 2) * 3 * LANES), BF16),
                pltpu.VMEM((samples, cols, rows, LANES), F32),
                pltpu.VMEM((4, 3, in_ch, 2 * LANES), BF16),
                pltpu.VMEM((in_ch, LANES), BF16),
                pltpu.VMEM((layers - 1, 4, 3, LANES, 2 * LANES), BF16),
                pltpu.VMEM((4 * cols, (cols + 2) * 3 * LANES), BF16),
                pltpu.VMEM((LANES, LANES), F32),
                pltpu.VMEM((LANES, LANES), F32),
                pltpu.VMEM((samples, 2 * halves, LANES), F32),
                pltpu.VMEM((layers, samples, 2, LANES), F32),
                pltpu.VMEM((samples, peers_n, 2 * halves, LANES), F32),
                pltpu.VMEM((layers, samples, peers_n, 2, LANES), F32),
                pltpu.VMEM((samples, 2, halves, cols, LANES), F32),
                pltpu.VMEM((layers, samples, 2, 1, cols, LANES), F32),
                pltpu.VMEM((samples, 2, 3, halves, cols, LANES), F32),
                pltpu.VMEM((layers, samples, 2, 3, 1, cols, LANES), F32),
                pltpu.SemaphoreType.DMA((samples,)),
                pltpu.SemaphoreType.DMA((layers + 1,)),
                pltpu.SemaphoreType.DMA((layers + 1, samples)),
                pltpu.SemaphoreType.DMA((layers + 1, samples)),
                pltpu.SemaphoreType.DMA((layers + 1, samples, 8)),
                pltpu.SemaphoreType.DMA((layers + 1, samples, 8)),
            ],
            compiler_params=pltpu.CompilerParams(collective_id=0, has_side_effects=True, vmem_limit_bytes=60 * 1024 * 1024),
            name="decode",
        )(act_in, w_first, w_short, w_rest, norm_first, norm_rest, bias_rest, jnp.transpose(w_out, (0, 1, 3, 2)))
        return jnp.transpose(image, (0, 3, 2, 1)) + bias_out.astype(F32)

    return jax.shard_map(local_decode, mesh=mesh, in_specs=(tile_spec,) + (replicated,) * 8, out_specs=tile_spec, check_vma=False)
```

```python
import functools

import jax
import jax.numpy as jnp
from jax import lax
from jax.experimental import pallas as pl
from jax.experimental.pallas import tpu as pltpu
from jax.sharding import PartitionSpec as P

GROUPS = 32
GN_EPS = 1e-6
LANES = 128
MESH = pl.DeviceIdType.MESH
F32 = jnp.float32
BF16 = jnp.bfloat16


def half_silu(half):
    return half + half * jnp.tanh(half)


def decode_kernel(rows_n, cols_n, act_hbm, w_first_hbm, w_short_hbm, w_rest_hbm, norm_first_hbm, norm_rest_hbm, bias_hbm, w_out_hbm, bias_out_ref, out_ref,
                  raw, flat, map_in, maps, z_in, z_mid, short, w_first, w_short, w_rest, w_head, ones_in, ones_mid,
                  norm_first_ref, norm_rest_ref, bias_ref, bias_rows, w_out_ref,
                  msg_in, msg_mid, got_in, got_mid, edge_in, edge_mid, halo_in, halo_mid, halo_act,
                  act_sem, weight_sem, small_sem, stat_recv, stat_send, halo_recv, halo_send):
    samples, rows, cols, in_ch = raw.shape
    halves = in_ch // LANES
    layers = w_rest.shape[0] + 1
    peers_n = rows_n * cols_n - 1
    sx = lax.axis_index("sx")
    sy = lax.axis_index("sy")
    core = lax.rem(sy, 2)
    chip = sy // 2
    chips_n = rows_n // 2

    def ring(offset, size):
        return min(offset, size - offset)

    offsets = [(dx, dy, dc) for dx in range(cols_n) for dy in range(chips_n) for dc in range(2) if (dx, dy, dc) != (0, 0, 0)]
    offsets.sort(key=lambda o: (-ring(o[0], cols_n) - ring(o[1], chips_n), o[2]))

    def peer(offset):
        dx, dy, dc = offset
        return {"sx": lax.rem(sx + dx, cols_n), "sy": lax.rem(chip + dy, chips_n) * 2 + (1 - core if dc else core)}

    barrier = pltpu.get_barrier_semaphore()
    for offset in offsets:
        pl.semaphore_signal(barrier, inc=1, device_id=peer(offset), device_id_type=MESH)

    for s in range(samples):
        pltpu.make_async_copy(act_hbm.at[s], raw.at[s], act_sem.at[s]).start()
    small = [(norm_first_hbm, norm_first_ref), (norm_rest_hbm, norm_rest_ref), (bias_hbm, bias_ref), (w_out_hbm, w_out_ref)]
    for at, (src, dst) in enumerate(small):
        pltpu.make_async_copy(src, dst, small_sem.at[at]).start()
    pltpu.make_async_copy(w_short_hbm, w_short, weight_sem.at[layers]).start()
    for o in range(2):
        for dc in range(3):
            pltpu.make_async_copy(w_first_hbm.at[:, dc], w_first.at[o + dc, :, :, pl.ds(o * LANES, LANES)], weight_sem.at[0]).start()

    has = {"up": sy > 0, "down": sy < rows_n - 1, "left": sx > 0, "right": sx < cols_n - 1}

    def both(one, two):
        return jnp.logical_and(has[one], has[two])

    row_moves = [
        (1, 1, 0, {"sy": sy - 1}, has["up"], has["down"]),
        (0, 1, 1, {"sy": sy + 1}, has["down"], has["up"]),
        (1, 2, 0, {"sx": sx - 1, "sy": sy - 1}, both("up", "left"), both("down", "right")),
        (1, 0, 0, {"sx": sx + 1, "sy": sy - 1}, both("up", "right"), both("down", "left")),
        (0, 2, 1, {"sx": sx - 1, "sy": sy + 1}, both("down", "left"), both("up", "right")),
        (0, 0, 1, {"sx": sx + 1, "sy": sy + 1}, both("down", "right"), both("up", "left")),
    ]

    def is_first(k):
        return isinstance(k, int) and k == 0

    def tile(k, s, c):
        return map_in.at[s, c] if is_first(k) else maps.at[k - 1, s, c]

    def edges(k, s):
        return edge_in.at[s] if is_first(k) else edge_mid.at[k - 1, s]

    def halo(k, s):
        return halo_in.at[s] if is_first(k) else halo_mid.at[k - 1, s]

    def message(k, s):
        return msg_in if is_first(k) else msg_mid.at[k - 1, s]

    def received(k, s):
        return got_in if is_first(k) else got_mid.at[k - 1, s]

    def col_copy(k, s, at):
        src, dst, to = ((1, cols + 1, {"sx": sx - 1}), (cols, 0, {"sx": sx + 1}))[at]
        return pltpu.make_async_remote_copy(tile(k, s, src), tile(k, s, dst), halo_send.at[k, s, at], halo_recv.at[k, s, at], device_id=to, device_id_type=MESH)

    def row_copy(k, s, at):
        side, place, edge, to, _, _ = row_moves[at]
        return pltpu.make_async_remote_copy(edges(k, s).at[edge], halo(k, s).at[side, place], halo_send.at[k, s, 2 + at], halo_recv.at[k, s, 2 + at], device_id=to, device_id_type=MESH)

    def send_cols(k, s):
        for at, there in enumerate((has["left"], has["right"])):
            pl.when(there)(lambda at=at: col_copy(k, s, at).start())

    def send_rows(k, s):
        for at, move in enumerate(row_moves):
            pl.when(move[4])(lambda at=at: row_copy(k, s, at).start())

    def send_stats(k, s):
        for slot, offset in enumerate(offsets):
            pltpu.make_async_remote_copy(message(k, s), received(k, s).at[slot], stat_send.at[k, s], stat_recv.at[k, s], device_id=peer(offset), device_id_type=MESH).start()

    def sent(k, s, first=None):
        if first is None:
            pltpu.make_async_copy(received(k, s), received(k, s), stat_send.at[k, s]).wait()
        for at, there in enumerate((has["left"], has["right"])):
            pl.when(there)(lambda at=at: col_copy(k, s, at).wait_send())
        for at, move in enumerate(row_moves):
            pl.when(move[4])(lambda at=at: row_copy(k, s, at).wait_send())

    def scales(k, s):
        if is_first(k):
            total = msg_in[s] + jnp.sum(got_in[:, s], axis=0)
        else:
            pltpu.make_async_copy(received(k, s), received(k, s), stat_recv.at[k, s]).wait()
            total = message(k, s)[...] + jnp.sum(received(k, s)[...], axis=0)
        ones = ones_in if is_first(k) else ones_mid
        total = jnp.dot(total, ones[...], precision=lax.Precision.HIGHEST, preferred_element_type=F32)
        parts = halves if is_first(k) else 1
        per_group = parts * LANES // GROUPS
        count = rows * rows_n * cols * cols_n * per_group
        rows_out = []
        for part in range(parts):
            norm = (norm_first_ref[:, part * LANES:(part + 1) * LANES] if is_first(k) else norm_rest_ref[k - 1]).astype(F32)
            mean = total[part:part + 1] / count
            square = total[parts + part:parts + part + 1] / count
            scale = lax.rsqrt(square - mean * mean + GN_EPS) * norm[0:1]
            shift = norm[1:2] - mean * scale
            rows_out.append((0.5 * scale, 0.5 * shift))
        return rows_out

    def activate_rows(k, s, scale_rows):
        for at, move in enumerate(row_moves):
            pl.when(move[5])(lambda at=at: row_copy(k, s, at).wait_recv())
        for part, (scale, shift) in enumerate(scale_rows):
            for side, there in ((0, "up"), (1, "down")):
                for place in range(3):
                    seen = has[there] if place == 1 else both(there, "left" if place == 0 else "right")
                    act = half_silu(halo(k, s)[side, place, part] * scale + shift)
                    halo_act[side, part, place * cols:(place + 1) * cols, :] = jnp.where(seen, act, 0.0)

    def activate(k, s, scale_rows, c):
        z = z_in if is_first(k) else z_mid
        parts = len(scale_rows)
        for part, (scale, shift) in enumerate(scale_rows):
            ref = map_in.at[s, c, part] if is_first(k) else maps.at[k - 1, s, c]
            act = half_silu(ref[...].astype(F32) * scale + shift)
            if c in (0, cols + 1):
                act = jnp.where(has["left" if c == 0 else "right"], act, 0.0)
            at = cols - 1 + c
            above = jnp.concatenate([halo_act[0, part, at:at + 1, :], act[:-1]], axis=0)
            below = jnp.concatenate([act[1:], halo_act[1, part, at:at + 1, :]], axis=0)
            for dr, value in enumerate((above, act, below)):
                z[(c * 3 + dr) * parts + part] = value.astype(BF16)

    def wait_cols(k, s):
        for at, there in enumerate((has["right"], has["left"])):
            pl.when(there)(lambda at=at: col_copy(k, s, at).wait_recv())

    def layer(k, s, skip):
        z = z_in if is_first(k) else z_mid
        scale_rows = scales(k, s)
        parts = len(scale_rows)
        depth = 3 * parts
        weights = (w_first[...] if is_first(k) else w_rest[k - 1]).reshape(4 * depth * LANES, 2 * LANES)
        bias = bias_rows[k]
        edge = edges(k + 1, s)

        def pair(p, sums):
            lhs = jnp.concatenate([z[2 * p * depth + i] for i in range(4 * depth)], axis=1)
            acc = jnp.dot(lhs, weights, preferred_element_type=F32)
            sum_one, sum_two = sums
            for o in range(2):
                c = 2 * p + o
                value = acc[:, o * LANES:(o + 1) * LANES] + bias
                if skip == "input":
                    value = value + short[s, c]
                elif skip == "map":
                    value = value + maps[k - 2, s, c + 1].astype(F32)
                rounded = value.astype(BF16)
                maps[k, s, c + 1] = rounded
                value = rounded.astype(F32)
                edge[0, 0, c:c + 1, :] = value[0:1]
                edge[1, 0, c:c + 1, :] = value[rows - 1:rows]
                value = value.reshape(rows // 8, 8, LANES)
                sum_one = sum_one + jnp.sum(value, axis=0)
                sum_two = sum_two + jnp.sum(value * value, axis=0)
            return sum_one, sum_two

        zero = jnp.zeros((8, LANES), F32)
        sums = (zero, zero)
        activate_rows(k, s, scale_rows)
        done = set()
        order = list(range(1, cols // 2 - 1)) + [0, cols // 2 - 1]
        for p in order:
            if p == 0:
                for c in range(1, cols + 1):
                    if c not in done:
                        activate(k, s, scale_rows, c)
                        done.add(c)
                wait_cols(k, s)
            for c in range(2 * p, 2 * p + 4):
                if c not in done:
                    activate(k, s, scale_rows, c)
                    done.add(c)
            sums = pair(p, sums)
        target = message(k + 1, s)
        for at, part in enumerate(sums):
            target[at:at + 1, :] = jnp.sum(part, axis=0, keepdims=True)
        send_stats(k + 1, s)
        send_rows(k + 1, s)
        send_cols(k + 1, s)
        sent(k, s, first=True if is_first(k) else None)

    chunk = 16

    def load(s):
        pltpu.make_async_copy(act_hbm.at[s], raw.at[s], act_sem.at[s]).wait()

        def step(i, sums):
            at = pl.multiple_of(i * chunk, chunk)
            sums = list(sums)
            for part in range(halves):
                value = raw[s, pl.ds(at, chunk), :, part * LANES:(part + 1) * LANES].astype(F32)
                flat[s, part, pl.ds(pl.multiple_of(at * cols, chunk * cols), chunk * cols), :] = value.reshape(chunk * cols, LANES)
                sums[part] = sums[part] + jnp.sum(value, axis=0)
                sums[halves + part] = sums[halves + part] + jnp.sum(value * value, axis=0)
            return tuple(sums)

        zero = jnp.zeros((cols, LANES), F32)
        sums = lax.fori_loop(0, rows // chunk, step, (zero,) * (2 * halves))
        for at, part in enumerate(sums):
            msg_in[s, at:at + 1, :] = jnp.sum(part, axis=0, keepdims=True)
        for part in range(halves):
            edge_in[s, 0, part] = flat[s, part, 0:cols, :]
            edge_in[s, 1, part] = flat[s, part, (rows - 1) * cols:, :]

    def turn(s, c):
        for part in range(halves):
            map_in[s, c + 1, part] = flat[s, part, pl.ds(c, rows, stride=cols), :].astype(BF16)

    for s in range(samples):
        load(s)
    pl.semaphore_wait(barrier, peers_n)
    send_stats(0, 0)
    for s in range(samples):
        turn(s, 0)
        turn(s, cols - 1)
        send_rows(0, s)
        send_cols(0, s)

    for k in range(layers - 1):
        for o in range(2):
            for dc in range(3):
                pltpu.make_async_copy(w_rest_hbm.at[k, :, dc], w_rest.at[k, o + dc, :, :, pl.ds(o * LANES, LANES)], weight_sem.at[k + 1]).start()
    for src_dst, at in zip(small, range(len(small))):
        pltpu.make_async_copy(*src_dst, small_sem.at[at]).wait()
    row_id = lax.broadcasted_iota(jnp.int32, (LANES, LANES), 0)
    lane_id = lax.broadcasted_iota(jnp.int32, (LANES, LANES), 1)
    for ones, per_group in ((ones_in, in_ch // GROUPS), (ones_mid, LANES // GROUPS)):
        ones[...] = jnp.where(row_id // per_group == lane_id // per_group, 1.0, 0.0).astype(F32)
    for dr in range(3):
        w_first[3, dr, :, 0:LANES] = jnp.zeros((in_ch, LANES), BF16)
        w_first[0, dr, :, LANES:] = jnp.zeros((in_ch, LANES), BF16)
    pltpu.make_async_copy(w_short_hbm, w_short, weight_sem.at[layers]).wait()
    for at in range(layers + 1):
        bias_rows[at] = bias_ref[at:at + 1].astype(F32)
    skip_bias = bias_rows[layers]
    def skip_product(s, _):
        for c in range(cols):
            if 0 < c < cols - 1:
                turn(s, c)
            both_halves = jnp.concatenate([map_in[s, c + 1, part] for part in range(halves)], axis=1)
            short[s, c] = jnp.dot(both_halves, w_short[...], preferred_element_type=F32) + skip_bias
        return 0

    lax.fori_loop(0, samples, skip_product, 0)

    def clear(k, _):
        for dr in range(3):
            w_rest[k, 3, dr, :, 0:LANES] = jnp.zeros((LANES, LANES), BF16)
            w_rest[k, 0, dr, :, LANES:] = jnp.zeros((LANES, LANES), BF16)
        return 0

    lax.fori_loop(0, layers - 1, clear, 0)

    col_id = lax.broadcasted_iota(jnp.int32, (cols, LANES), 0)

    def head_block(j, _):
        for dr in range(3):
            blocks = []
            for ch in range(3):
                block = jnp.zeros((cols, LANES), F32)
                for dc in range(3):
                    block = jnp.where(col_id == j - dc, w_out_ref[dr, dc, ch:ch + 1, :].astype(F32), block)
                blocks.append(block)
            blocks.append(jnp.zeros((cols, LANES), F32))
            w_head[:, pl.ds(pl.multiple_of((j * 3 + dr) * LANES, LANES), LANES)] = jnp.concatenate(blocks, axis=0).astype(BF16)
        return 0

    lax.fori_loop(0, cols + 2, head_block, 0)

    def both_samples(k, skip):
        lax.fori_loop(0, samples, lambda s, _: (layer(k, s, skip), 0)[1], 0)

    def weights_here(k):
        pltpu.make_async_copy(w_rest.at[k - 1, 0:3], w_rest.at[k - 1, 0:3], weight_sem.at[k]).wait()

    pltpu.make_async_copy(w_first.at[0:3], w_first.at[0:3], weight_sem.at[0]).wait()
    pltpu.make_async_copy(got_in, got_in, stat_recv.at[0, 0]).wait()
    both_samples(0, None)
    pltpu.make_async_copy(got_in, got_in, stat_send.at[0, 0]).wait()
    weights_here(1)
    both_samples(1, "input")

    def block(i, _):
        weights_here(2 * i)
        both_samples(2 * i, None)
        weights_here(2 * i + 1)
        both_samples(2 * i + 1, "map")
        return 0

    lax.fori_loop(1, layers // 2, block, 0)

    def head(s, _):
        scale_rows = scales(layers, s)
        activate_rows(layers, s, scale_rows)
        for c in range(1, cols + 1):
            activate(layers, s, scale_rows, c)
        wait_cols(layers, s)
        activate(layers, s, scale_rows, 0)
        activate(layers, s, scale_rows, cols + 1)
        acts = jnp.concatenate([z_mid[i] for i in range(3 * (cols + 2))], axis=1)
        rgb = lax.dot_general(w_head[...], acts, (((1,), (1,)), ((), ())), preferred_element_type=F32)
        for ch in range(3):
            out_ref[s, ch] = rgb[ch * cols:(ch + 1) * cols] + bias_out_ref[:, ch:ch + 1].astype(F32)
        sent(layers, s)
        return 0

    lax.fori_loop(0, samples, head, 0)


def solution(mesh):
    rows_n = mesh.shape["sy"]
    cols_n = mesh.shape["sx"]
    tile_spec = P("dp", "sy", "sx", None)
    replicated = P()

    def local_decode(act_in, norm_first, w_first, w_short, norm_rest, w_rest, bias_rest, w_out, bias_out):
        samples, rows, cols, in_ch = act_in.shape
        halves = in_ch // LANES
        layers = w_rest.shape[0] + 1
        peers_n = rows_n * cols_n - 1
        anywhere = pl.BlockSpec(memory_space=pl.ANY)
        in_vmem = pl.BlockSpec(memory_space=pltpu.VMEM)
        image = pl.pallas_call(
            functools.partial(decode_kernel, rows_n, cols_n),
            out_shape=jax.ShapeDtypeStruct((samples, 3, cols, rows), F32),
            in_specs=[anywhere] * 8 + [in_vmem],
            out_specs=in_vmem,
            scratch_shapes=[
                pltpu.VMEM((samples, rows, cols, in_ch), BF16),
                pltpu.VMEM((samples, halves, rows * cols, LANES), F32),
                pltpu.VMEM((samples, cols + 2, halves, rows, LANES), BF16),
                pltpu.VMEM((layers, samples, cols + 2, rows, LANES), BF16),
                pltpu.VMEM(((cols + 2) * 3 * halves, rows, LANES), BF16),
                pltpu.VMEM(((cols + 2) * 3, rows, LANES), BF16),
                pltpu.VMEM((samples, cols, rows, LANES), F32),
                pltpu.VMEM((4, 3, in_ch, 2 * LANES), BF16),
                pltpu.VMEM((in_ch, LANES), BF16),
                pltpu.VMEM((layers - 1, 4, 3, LANES, 2 * LANES), BF16),
                pltpu.VMEM((4 * cols, (cols + 2) * 3 * LANES), BF16),
                pltpu.VMEM((LANES, LANES), F32),
                pltpu.VMEM((LANES, LANES), F32),
                pltpu.VMEM(norm_first.shape, BF16),
                pltpu.VMEM(norm_rest.shape, BF16),
                pltpu.VMEM(bias_rest.shape, BF16),
                pltpu.VMEM((bias_rest.shape[0], 1, LANES), F32),
                pltpu.VMEM((3, 3, 3, LANES), BF16),
                pltpu.VMEM((samples, 2 * halves, LANES), F32),
                pltpu.VMEM((layers, samples, 2, LANES), F32),
                pltpu.VMEM((peers_n, samples, 2 * halves, LANES), F32),
                pltpu.VMEM((layers, samples, peers_n, 2, LANES), F32),
                pltpu.VMEM((samples, 2, halves, cols, LANES), F32),
                pltpu.VMEM((layers, samples, 2, 1, cols, LANES), F32),
                pltpu.VMEM((samples, 2, 3, halves, cols, LANES), F32),
                pltpu.VMEM((layers, samples, 2, 3, 1, cols, LANES), F32),
                pltpu.VMEM((2, halves, 3 * cols, LANES), F32),
                pltpu.SemaphoreType.DMA((samples,)),
                pltpu.SemaphoreType.DMA((layers + 1,)),
                pltpu.SemaphoreType.DMA((4,)),
                pltpu.SemaphoreType.DMA((layers + 1, samples)),
                pltpu.SemaphoreType.DMA((layers + 1, samples)),
                pltpu.SemaphoreType.DMA((layers + 1, samples, 8)),
                pltpu.SemaphoreType.DMA((layers + 1, samples, 8)),
            ],
            compiler_params=pltpu.CompilerParams(collective_id=0, has_side_effects=True, vmem_limit_bytes=60 * 1024 * 1024),
            name="decode",
        )(act_in, w_first, w_short, w_rest, norm_first, norm_rest, bias_rest, jnp.transpose(w_out, (0, 1, 3, 2)), bias_out.reshape(1, 3))
        return jnp.transpose(image, (0, 3, 2, 1))

    return jax.shard_map(local_decode, mesh=mesh, in_specs=(tile_spec,) + (replicated,) * 8, out_specs=tile_spec, check_vma=False)
```

```python
import functools

import jax
import jax.numpy as jnp
from jax import lax
from jax.experimental import pallas as pl
from jax.experimental.pallas import tpu as pltpu
from jax.sharding import PartitionSpec as P

GROUPS = 32
GN_EPS = 1e-6
LANES = 128
MESH = pl.DeviceIdType.MESH
F32 = jnp.float32
BF16 = jnp.bfloat16


def half_silu(half):
    return half + half * jnp.tanh(half)


def decode_kernel(rows_n, cols_n, act_hbm, w_first_hbm, w_short_hbm, w_rest_hbm, norm_first_hbm, norm_rest_hbm, bias_hbm, w_out_hbm, bias_out_ref, out_ref,
                  raw, flat, map_in, mid_maps, hidden_maps, z_in, z_mid, short, w_first, w_short, w_rest, w_head, ones_in, ones_mid,
                  norm_first_ref, norm_rest_ref, bias_ref, bias_rows, w_out_ref,
                  msg_in, msg_mid, got_in, got_mid, edge_in, edge_mid, halo_in, halo_mid, halo_act,
                  act_sem, weight_sem, small_sem, stat_recv, stat_send, halo_recv, halo_send):
    samples, rows, cols, in_ch = raw.shape
    halves = in_ch // LANES
    layers = w_rest.shape[0] + 1
    peers_n = rows_n * cols_n - 1
    sx = lax.axis_index("sx")
    sy = lax.axis_index("sy")
    core = lax.rem(sy, 2)
    chip = sy // 2
    chips_n = rows_n // 2

    def ring(offset, size):
        return min(offset, size - offset)

    offsets = [(dx, dy, dc) for dx in range(cols_n) for dy in range(chips_n) for dc in range(2) if (dx, dy, dc) != (0, 0, 0)]
    offsets.sort(key=lambda o: (-ring(o[0], cols_n) - ring(o[1], chips_n), o[2]))

    def peer(offset):
        dx, dy, dc = offset
        return {"sx": lax.rem(sx + dx, cols_n), "sy": lax.rem(chip + dy, chips_n) * 2 + (1 - core if dc else core)}

    barrier = pltpu.get_barrier_semaphore()
    for offset in offsets:
        pl.semaphore_signal(barrier, inc=1, device_id=peer(offset), device_id_type=MESH)

    for s in range(samples):
        pltpu.make_async_copy(act_hbm.at[s], raw.at[s], act_sem.at[s]).start()
    small = [(norm_first_hbm, norm_first_ref), (norm_rest_hbm, norm_rest_ref), (bias_hbm, bias_ref), (w_out_hbm, w_out_ref)]
    for at, (src, dst) in enumerate(small):
        pltpu.make_async_copy(src, dst, small_sem.at[at]).start()
    pltpu.make_async_copy(w_short_hbm, w_short, weight_sem.at[layers]).start()
    for o in range(2):
        for dc in range(3):
            pltpu.make_async_copy(w_first_hbm.at[:, dc], w_first.at[o + dc, :, :, pl.ds(o * LANES, LANES)], weight_sem.at[0]).start()

    has = {"up": sy > 0, "down": sy < rows_n - 1, "left": sx > 0, "right": sx < cols_n - 1}

    def both(one, two):
        return jnp.logical_and(has[one], has[two])

    row_moves = [
        (1, 1, 0, {"sy": sy - 1}, has["up"], has["down"]),
        (0, 1, 1, {"sy": sy + 1}, has["down"], has["up"]),
        (1, 2, 0, {"sx": sx - 1, "sy": sy - 1}, both("up", "left"), both("down", "right")),
        (1, 0, 0, {"sx": sx + 1, "sy": sy - 1}, both("up", "right"), both("down", "left")),
        (0, 2, 1, {"sx": sx - 1, "sy": sy + 1}, both("down", "left"), both("up", "right")),
        (0, 0, 1, {"sx": sx + 1, "sy": sy + 1}, both("down", "right"), both("up", "left")),
    ]

    def is_first(k):
        return k[1] == 0 and isinstance(k[0], int) and k[0] == 0

    def number(k):
        return 2 * k[0] + k[1]

    def following(k):
        return (k[0], 1) if k[1] == 0 else (k[0] + 1, 0)

    def tile(k, s, c):
        if is_first(k):
            return map_in.at[s, c]
        return mid_maps.at[k[0], s, c] if k[1] else hidden_maps.at[k[0] - 1, s, c]

    def edges(k, s):
        return edge_in.at[s] if is_first(k) else edge_mid.at[number(k) - 1, s]

    def halo(k, s):
        return halo_in.at[s] if is_first(k) else halo_mid.at[number(k) - 1, s]

    def message(k, s):
        return msg_in if is_first(k) else msg_mid.at[number(k) - 1, s]

    def received(k, s):
        return got_in if is_first(k) else got_mid.at[number(k) - 1, s]

    def col_copy(k, s, at):
        src, dst, to = ((1, cols + 1, {"sx": sx - 1}), (cols, 0, {"sx": sx + 1}))[at]
        return pltpu.make_async_remote_copy(tile(k, s, src), tile(k, s, dst), halo_send.at[number(k), s, at], halo_recv.at[number(k), s, at], device_id=to, device_id_type=MESH)

    def row_copy(k, s, at):
        side, place, edge, to, _, _ = row_moves[at]
        return pltpu.make_async_remote_copy(edges(k, s).at[edge], halo(k, s).at[side, place], halo_send.at[number(k), s, 2 + at], halo_recv.at[number(k), s, 2 + at], device_id=to, device_id_type=MESH)

    def send_cols(k, s):
        for at, there in enumerate((has["left"], has["right"])):
            pl.when(there)(lambda at=at: col_copy(k, s, at).start())

    def send_rows(k, s):
        for at, move in enumerate(row_moves):
            pl.when(move[4])(lambda at=at: row_copy(k, s, at).start())

    def send_stats(k, s):
        for slot, offset in enumerate(offsets):
            pltpu.make_async_remote_copy(message(k, s), received(k, s).at[slot], stat_send.at[number(k), s], stat_recv.at[number(k), s], device_id=peer(offset), device_id_type=MESH).start()

    def sent(k, s, first=None):
        if first is None:
            pltpu.make_async_copy(received(k, s), received(k, s), stat_send.at[number(k), s]).wait()
        for at, there in enumerate((has["left"], has["right"])):
            pl.when(there)(lambda at=at: col_copy(k, s, at).wait_send())
        for at, move in enumerate(row_moves):
            pl.when(move[4])(lambda at=at: row_copy(k, s, at).wait_send())

    def scales(k, s):
        if is_first(k):
            total = msg_in[s] + jnp.sum(got_in[:, s], axis=0)
        else:
            pltpu.make_async_copy(received(k, s), received(k, s), stat_recv.at[number(k), s]).wait()
            total = message(k, s)[...] + jnp.sum(received(k, s)[...], axis=0)
        ones = ones_in if is_first(k) else ones_mid
        high = total.astype(BF16)
        rest = total - high.astype(F32)
        middle = rest.astype(BF16)
        low = (rest - middle.astype(F32)).astype(BF16)
        total = sum(jnp.dot(piece, ones[...], preferred_element_type=F32) for piece in (low, middle, high))
        parts = halves if is_first(k) else 1
        per_group = parts * LANES // GROUPS
        count = rows * rows_n * cols * cols_n * per_group
        rows_out = []
        for part in range(parts):
            norm = (norm_first_ref[:, part * LANES:(part + 1) * LANES] if is_first(k) else norm_rest_ref[number(k) - 1]).astype(F32)
            mean = total[part:part + 1] / count
            square = total[parts + part:parts + part + 1] / count
            scale = lax.rsqrt(square - mean * mean + GN_EPS) * norm[0:1]
            shift = norm[1:2] - mean * scale
            rows_out.append((0.5 * scale, 0.5 * shift))
        return rows_out

    def activate_rows(k, s, scale_rows):
        for at, move in enumerate(row_moves):
            pl.when(move[5])(lambda at=at: row_copy(k, s, at).wait_recv())
        for part, (scale, shift) in enumerate(scale_rows):
            for side, there in ((0, "up"), (1, "down")):
                for place in range(3):
                    seen = has[there] if place == 1 else both(there, "left" if place == 0 else "right")
                    act = half_silu(halo(k, s)[side, place, part] * scale + shift)
                    halo_act[side, part, place * cols:(place + 1) * cols, :] = jnp.where(seen, act, 0.0)

    def activate(k, s, scale_rows, c):
        z = z_in if is_first(k) else z_mid
        parts = len(scale_rows)
        for part, (scale, shift) in enumerate(scale_rows):
            ref = tile(k, s, c).at[part] if is_first(k) else tile(k, s, c)
            act = half_silu(ref[...].astype(F32) * scale + shift)
            if c in (0, cols + 1):
                act = jnp.where(has["left" if c == 0 else "right"], act, 0.0)
            at = cols - 1 + c
            above = jnp.concatenate([halo_act[0, part, at:at + 1, :], act[:-1]], axis=0)
            below = jnp.concatenate([act[1:], halo_act[1, part, at:at + 1, :]], axis=0)
            for dr, value in enumerate((above, act, below)):
                z[(c * 3 + dr) * parts + part] = value.astype(BF16)

    def wait_cols(k, s):
        for at, there in enumerate((has["right"], has["left"])):
            pl.when(there)(lambda at=at: col_copy(k, s, at).wait_recv())

    def layer(k, s):
        z = z_in if is_first(k) else z_mid
        scale_rows = scales(k, s)
        parts = len(scale_rows)
        depth = 3 * parts
        weights = (w_first[...] if is_first(k) else w_rest[number(k) - 1]).reshape(4 * depth * LANES, 2 * LANES)
        bias = bias_rows[number(k)]
        later = following(k)
        edge = edges(later, s)

        def pair(p, sums):
            lhs = jnp.concatenate([z[2 * p * depth + i] for i in range(4 * depth)], axis=1)
            acc = jnp.dot(lhs, weights, preferred_element_type=F32)
            sum_one, sum_two = sums
            for o in range(2):
                c = 2 * p + o
                value = acc[:, o * LANES:(o + 1) * LANES] + bias
                if k[1]:
                    value = value + short[s, c]
                rounded = value.astype(BF16)
                tile(later, s, c + 1)[...] = rounded
                value = rounded.astype(F32)
                if k[1]:
                    short[s, c] = value
                edge[0, 0, c:c + 1, :] = value[0:1]
                edge[1, 0, c:c + 1, :] = value[rows - 1:rows]
                value = value.reshape(rows // 8, 8, LANES)
                sum_one = sum_one + jnp.sum(value, axis=0)
                sum_two = sum_two + jnp.sum(value * value, axis=0)
            return sum_one, sum_two

        zero = jnp.zeros((8, LANES), F32)
        sums = (zero, zero)
        activate_rows(k, s, scale_rows)
        done = set()
        order = list(range(1, cols // 2 - 1)) + [0, cols // 2 - 1]
        for p in order:
            if p == 0:
                for c in range(1, cols + 1):
                    if c not in done:
                        activate(k, s, scale_rows, c)
                        done.add(c)
                wait_cols(k, s)
            for c in range(2 * p, 2 * p + 4):
                if c not in done:
                    activate(k, s, scale_rows, c)
                    done.add(c)
            sums = pair(p, sums)
        target = message(later, s)
        for at, part in enumerate(sums):
            target[at:at + 1, :] = jnp.sum(part, axis=0, keepdims=True)
        send_stats(later, s)
        send_rows(later, s)
        send_cols(later, s)
        sent(k, s, first=True if is_first(k) else None)

    chunk = 16

    def load(s):
        pltpu.make_async_copy(act_hbm.at[s], raw.at[s], act_sem.at[s]).wait()

        def step(i, sums):
            at = pl.multiple_of(i * chunk, chunk)
            sums = list(sums)
            for part in range(halves):
                value = raw[s, pl.ds(at, chunk), :, part * LANES:(part + 1) * LANES].astype(F32)
                flat[s, part, pl.ds(pl.multiple_of(at * cols, chunk * cols), chunk * cols), :] = value.reshape(chunk * cols, LANES)
                sums[part] = sums[part] + jnp.sum(value, axis=0)
                sums[halves + part] = sums[halves + part] + jnp.sum(value * value, axis=0)
            return tuple(sums)

        zero = jnp.zeros((cols, LANES), F32)
        sums = lax.fori_loop(0, rows // chunk, step, (zero,) * (2 * halves))
        for at, part in enumerate(sums):
            msg_in[s, at:at + 1, :] = jnp.sum(part, axis=0, keepdims=True)
        for part in range(halves):
            edge_in[s, 0, part] = flat[s, part, 0:cols, :]
            edge_in[s, 1, part] = flat[s, part, (rows - 1) * cols:, :]

    def turn(s, c):
        for part in range(halves):
            map_in[s, c + 1, part] = flat[s, part, pl.ds(c, rows, stride=cols), :].astype(BF16)

    first = (0, 0)
    for s in range(samples):
        load(s)
    for s in range(samples):
        turn(s, 0)
        turn(s, cols - 1)
    pl.semaphore_wait(barrier, peers_n)
    send_stats(first, 0)
    for s in range(samples):
        send_rows(first, s)
        send_cols(first, s)

    for k in range(layers - 1):
        for o in range(2):
            for dc in range(3):
                pltpu.make_async_copy(w_rest_hbm.at[k, :, dc], w_rest.at[k, o + dc, :, :, pl.ds(o * LANES, LANES)], weight_sem.at[k + 1]).start()
    for src_dst, at in zip(small, range(len(small))):
        pltpu.make_async_copy(*src_dst, small_sem.at[at]).wait()
    row_id = lax.broadcasted_iota(jnp.int32, (LANES, LANES), 0)
    lane_id = lax.broadcasted_iota(jnp.int32, (LANES, LANES), 1)
    for ones, per_group in ((ones_in, in_ch // GROUPS), (ones_mid, LANES // GROUPS)):
        ones[...] = jnp.where(row_id // per_group == lane_id // per_group, 1.0, 0.0).astype(BF16)
    for dr in range(3):
        w_first[3, dr, :, 0:LANES] = jnp.zeros((in_ch, LANES), BF16)
        w_first[0, dr, :, LANES:] = jnp.zeros((in_ch, LANES), BF16)
    pltpu.make_async_copy(w_short_hbm, w_short, weight_sem.at[layers]).wait()
    for at in range(layers + 1):
        bias_rows[at] = bias_ref[at:at + 1].astype(F32)
    skip_bias = bias_rows[layers]
    def skip_product(s, _):
        for c in range(cols):
            if 0 < c < cols - 1:
                turn(s, c)
            both_halves = jnp.concatenate([map_in[s, c + 1, part] for part in range(halves)], axis=1)
            short[s, c] = jnp.dot(both_halves, w_short[...], preferred_element_type=F32) + skip_bias
        return 0

    lax.fori_loop(0, samples, skip_product, 0)

    def clear(k, _):
        for dr in range(3):
            w_rest[k, 3, dr, :, 0:LANES] = jnp.zeros((LANES, LANES), BF16)
            w_rest[k, 0, dr, :, LANES:] = jnp.zeros((LANES, LANES), BF16)
        return 0

    lax.fori_loop(0, layers - 1, clear, 0)

    col_id = lax.broadcasted_iota(jnp.int32, (cols, LANES), 0)

    def head_block(j, _):
        for dr in range(3):
            blocks = []
            for ch in range(3):
                block = jnp.zeros((cols, LANES), F32)
                for dc in range(3):
                    block = jnp.where(col_id == j - dc, w_out_ref[dr, dc, ch:ch + 1, :].astype(F32), block)
                blocks.append(block)
            blocks.append(jnp.zeros((cols, LANES), F32))
            w_head[:, pl.ds(pl.multiple_of((j * 3 + dr) * LANES, LANES), LANES)] = jnp.concatenate(blocks, axis=0).astype(BF16)
        return 0

    lax.fori_loop(0, cols + 2, head_block, 0)

    def both_samples(k):
        if not is_first(k):
            at = number(k) - 1
            pltpu.make_async_copy(w_rest.at[at, 0:3], w_rest.at[at, 0:3], weight_sem.at[at + 1]).wait()
        lax.fori_loop(0, samples, lambda s, _: (layer(k, s), 0)[1], 0)

    pltpu.make_async_copy(w_first.at[0:3], w_first.at[0:3], weight_sem.at[0]).wait()
    pltpu.make_async_copy(got_in, got_in, stat_recv.at[0, 0]).wait()
    both_samples(first)
    pltpu.make_async_copy(got_in, got_in, stat_send.at[0, 0]).wait()
    both_samples((0, 1))

    def block(i, _):
        both_samples((i, 0))
        both_samples((i, 1))
        return 0

    lax.fori_loop(1, layers // 2, block, 0)
    last = (layers // 2, 0)

    def head(s, _):
        scale_rows = scales(last, s)
        activate_rows(last, s, scale_rows)

        def product(blocks):
            acts = jnp.concatenate([z_mid[i] for i in blocks], axis=1)
            weights = w_head[:, blocks[0] * LANES:(blocks[-1] + 1) * LANES]
            return lax.dot_general(weights, acts, (((1,), (1,)), ((), ())), preferred_element_type=F32)

        for c in range(1, cols + 1):
            activate(last, s, scale_rows, c)
        rgb = product(range(3, 3 * (cols + 1)))
        wait_cols(last, s)
        for c in (0, cols + 1):
            activate(last, s, scale_rows, c)
            rgb = rgb + product(range(3 * c, 3 * c + 3))
        for ch in range(3):
            out_ref[s, ch] = rgb[ch * cols:(ch + 1) * cols] + bias_out_ref[:, ch:ch + 1].astype(F32)
        sent(last, s)
        return 0

    lax.fori_loop(0, samples, head, 0)


def solution(mesh):
    rows_n = mesh.shape["sy"]
    cols_n = mesh.shape["sx"]
    tile_spec = P("dp", "sy", "sx", None)
    replicated = P()

    def local_decode(act_in, norm_first, w_first, w_short, norm_rest, w_rest, bias_rest, w_out, bias_out):
        samples, rows, cols, in_ch = act_in.shape
        halves = in_ch // LANES
        layers = w_rest.shape[0] + 1
        peers_n = rows_n * cols_n - 1
        anywhere = pl.BlockSpec(memory_space=pl.ANY)
        in_vmem = pl.BlockSpec(memory_space=pltpu.VMEM)
        image = pl.pallas_call(
            functools.partial(decode_kernel, rows_n, cols_n),
            out_shape=jax.ShapeDtypeStruct((samples, 3, cols, rows), F32),
            in_specs=[anywhere] * 8 + [in_vmem],
            out_specs=in_vmem,
            scratch_shapes=[
                pltpu.VMEM((samples, rows, cols, in_ch), BF16),
                pltpu.VMEM((samples, halves, rows * cols, LANES), F32),
                pltpu.VMEM((samples, cols + 2, halves, rows, LANES), BF16),
                pltpu.VMEM(((layers + 1) // 2, samples, cols + 2, rows, LANES), BF16),
                pltpu.VMEM(((layers + 1) // 2, samples, cols + 2, rows, LANES), BF16),
                pltpu.VMEM(((cols + 2) * 3 * halves, rows, LANES), BF16),
                pltpu.VMEM(((cols + 2) * 3, rows, LANES), BF16),
                pltpu.VMEM((samples, cols, rows, LANES), F32),
                pltpu.VMEM((4, 3, in_ch, 2 * LANES), BF16),
                pltpu.VMEM((in_ch, LANES), BF16),
                pltpu.VMEM((layers - 1, 4, 3, LANES, 2 * LANES), BF16),
                pltpu.VMEM((4 * cols, (cols + 2) * 3 * LANES), BF16),
                pltpu.VMEM((LANES, LANES), BF16),
                pltpu.VMEM((LANES, LANES), BF16),
                pltpu.VMEM(norm_first.shape, BF16),
                pltpu.VMEM(norm_rest.shape, BF16),
                pltpu.VMEM(bias_rest.shape, BF16),
                pltpu.VMEM((bias_rest.shape[0], 1, LANES), F32),
                pltpu.VMEM((3, 3, 3, LANES), BF16),
                pltpu.VMEM((samples, 2 * halves, LANES), F32),
                pltpu.VMEM((layers, samples, 2, LANES), F32),
                pltpu.VMEM((peers_n, samples, 2 * halves, LANES), F32),
                pltpu.VMEM((layers, samples, peers_n, 2, LANES), F32),
                pltpu.VMEM((samples, 2, halves, cols, LANES), F32),
                pltpu.VMEM((layers, samples, 2, 1, cols, LANES), F32),
                pltpu.VMEM((samples, 2, 3, halves, cols, LANES), F32),
                pltpu.VMEM((layers, samples, 2, 3, 1, cols, LANES), F32),
                pltpu.VMEM((2, halves, 3 * cols, LANES), F32),
                pltpu.SemaphoreType.DMA((samples,)),
                pltpu.SemaphoreType.DMA((layers + 1,)),
                pltpu.SemaphoreType.DMA((4,)),
                pltpu.SemaphoreType.DMA((layers + 1, samples)),
                pltpu.SemaphoreType.DMA((layers + 1, samples)),
                pltpu.SemaphoreType.DMA((layers + 1, samples, 8)),
                pltpu.SemaphoreType.DMA((layers + 1, samples, 8)),
            ],
            compiler_params=pltpu.CompilerParams(collective_id=0, has_side_effects=True, vmem_limit_bytes=60 * 1024 * 1024),
            name="decode",
        )(act_in, w_first, w_short, w_rest, norm_first, norm_rest, bias_rest, jnp.transpose(w_out, (0, 1, 3, 2)), bias_out.reshape(1, 3))
        return jnp.transpose(image, (0, 3, 2, 1))

    return jax.shard_map(local_decode, mesh=mesh, in_specs=(tile_spec,) + (replicated,) * 8, out_specs=tile_spec, check_vma=False)
```

```python
import functools

import jax
import jax.numpy as jnp
from jax import lax
from jax.experimental import pallas as pl
from jax.experimental.pallas import tpu as pltpu
from jax.sharding import PartitionSpec as P

GROUPS = 32
GN_EPS = 1e-6
LANES = 128
MESH = pl.DeviceIdType.MESH
F32 = jnp.float32
BF16 = jnp.bfloat16


def half_silu(half):
    return half + half * jnp.tanh(half)


def decode_kernel(rows_n, cols_n, act_hbm, w_first_hbm, w_short_hbm, w_rest_hbm, norm_first_hbm, norm_rest_hbm, bias_hbm, w_out_hbm, bias_out_hbm, out_ref,
                  raw, flat, map_in, mid_maps, hidden_maps, z_in, z_mid, short, w_first, w_short, w_rest, w_head, ones_in, ones_mid,
                  norm_first_ref, norm_rest_ref, bias_ref, bias_rows, w_out_ref, bias_out_ref,
                  msg_in, msg_mid, got_in, got_mid, edge_in, edge_mid, halo_in, halo_mid, halo_act,
                  act_sem, weight_sem, small_sem, stat_recv, stat_send, halo_recv, halo_send):
    samples, rows, cols, in_ch = raw.shape
    halves = in_ch // LANES
    layers = w_rest.shape[0] + 1
    peers_n = rows_n * cols_n - 1
    sx = lax.axis_index("sx")
    sy = lax.axis_index("sy")
    core = lax.rem(sy, 2)
    chip = sy // 2
    chips_n = rows_n // 2

    def ring(offset, size):
        return min(offset, size - offset)

    offsets = [(dx, dy, dc) for dx in range(cols_n) for dy in range(chips_n) for dc in range(2) if (dx, dy, dc) != (0, 0, 0)]
    offsets.sort(key=lambda o: (-ring(o[0], cols_n) - ring(o[1], chips_n), o[2]))

    def peer(offset):
        dx, dy, dc = offset
        return {"sx": lax.rem(sx + dx, cols_n), "sy": lax.rem(chip + dy, chips_n) * 2 + (1 - core if dc else core)}

    barrier = pltpu.get_barrier_semaphore()
    for offset in offsets:
        pl.semaphore_signal(barrier, inc=1, device_id=peer(offset), device_id_type=MESH)

    for s in range(samples):
        pltpu.make_async_copy(act_hbm.at[s], raw.at[s], act_sem.at[s]).start()
    small = [(norm_first_hbm, norm_first_ref), (norm_rest_hbm, norm_rest_ref), (bias_hbm, bias_ref), (w_out_hbm, w_out_ref), (bias_out_hbm, bias_out_ref)]
    for at, (src, dst) in enumerate(small):
        pltpu.make_async_copy(src, dst, small_sem.at[at]).start()
    pltpu.make_async_copy(w_short_hbm, w_short, weight_sem.at[layers]).start()
    for o in range(2):
        for dc in range(3):
            pltpu.make_async_copy(w_first_hbm.at[:, dc], w_first.at[o + dc, :, :, pl.ds(o * LANES, LANES)], weight_sem.at[0]).start()

    has = {"up": sy > 0, "down": sy < rows_n - 1, "left": sx > 0, "right": sx < cols_n - 1}

    def both(one, two):
        return jnp.logical_and(has[one], has[two])

    row_moves = [
        (1, 1, 0, {"sy": sy - 1}, has["up"], has["down"]),
        (0, 1, 1, {"sy": sy + 1}, has["down"], has["up"]),
        (1, 2, 0, {"sx": sx - 1, "sy": sy - 1}, both("up", "left"), both("down", "right")),
        (1, 0, 0, {"sx": sx + 1, "sy": sy - 1}, both("up", "right"), both("down", "left")),
        (0, 2, 1, {"sx": sx - 1, "sy": sy + 1}, both("down", "left"), both("up", "right")),
        (0, 0, 1, {"sx": sx + 1, "sy": sy + 1}, both("down", "right"), both("up", "left")),
    ]

    def is_first(k):
        return k[1] == 0 and isinstance(k[0], int) and k[0] == 0

    def number(k):
        return 2 * k[0] + k[1]

    def following(k):
        return (k[0], 1) if k[1] == 0 else (k[0] + 1, 0)

    def tile(k, s, c):
        if is_first(k):
            return map_in.at[s, c]
        return mid_maps.at[k[0], s, c] if k[1] else hidden_maps.at[k[0] - 1, s, c]

    def edges(k, s):
        return edge_in.at[s] if is_first(k) else edge_mid.at[number(k) - 1, s]

    def halo(k, s):
        return halo_in.at[s] if is_first(k) else halo_mid.at[number(k) - 1, s]

    def message(k, s):
        return msg_in if is_first(k) else msg_mid.at[number(k) - 1, s]

    def received(k, s):
        return got_in if is_first(k) else got_mid.at[number(k) - 1, s]

    def col_copy(k, s, at):
        src, dst, to = ((1, cols + 1, {"sx": sx - 1}), (cols, 0, {"sx": sx + 1}))[at]
        return pltpu.make_async_remote_copy(tile(k, s, src), tile(k, s, dst), halo_send.at[number(k), s, at], halo_recv.at[number(k), s, at], device_id=to, device_id_type=MESH)

    def row_copy(k, s, at):
        side, place, edge, to, _, _ = row_moves[at]
        return pltpu.make_async_remote_copy(edges(k, s).at[edge], halo(k, s).at[side, place], halo_send.at[number(k), s, 2 + at], halo_recv.at[number(k), s, 2 + at], device_id=to, device_id_type=MESH)

    def send_cols(k, s):
        for at, there in enumerate((has["left"], has["right"])):
            pl.when(there)(lambda at=at: col_copy(k, s, at).start())

    def send_rows(k, s):
        for at, move in enumerate(row_moves):
            pl.when(move[4])(lambda at=at: row_copy(k, s, at).start())

    def send_stats(k, s):
        for slot, offset in enumerate(offsets):
            pltpu.make_async_remote_copy(message(k, s), received(k, s).at[slot], stat_send.at[number(k), s], stat_recv.at[number(k), s], device_id=peer(offset), device_id_type=MESH).start()

    def sent(k, s, first=None):
        if first is None:
            pltpu.make_async_copy(received(k, s), received(k, s), stat_send.at[number(k), s]).wait()
        for at, there in enumerate((has["left"], has["right"])):
            pl.when(there)(lambda at=at: col_copy(k, s, at).wait_send())
        for at, move in enumerate(row_moves):
            pl.when(move[4])(lambda at=at: row_copy(k, s, at).wait_send())

    def wait_rows(k, s):
        for at, move in enumerate(row_moves):
            pl.when(move[5])(lambda at=at: row_copy(k, s, at).wait_recv())

    def scales(k, s):
        wait_rows(k, s)
        if is_first(k):
            total = msg_in[s] + jnp.sum(got_in[:, s], axis=0)
        else:
            wait_cols(k, s)
            pltpu.make_async_copy(received(k, s), received(k, s), stat_recv.at[number(k), s]).wait()
            total = message(k, s)[...] + jnp.sum(received(k, s)[...], axis=0)
        ones = ones_in if is_first(k) else ones_mid
        high = total.astype(BF16)
        rest = total - high.astype(F32)
        middle = rest.astype(BF16)
        low = (rest - middle.astype(F32)).astype(BF16)
        total = sum(jnp.dot(piece, ones[...], preferred_element_type=F32) for piece in (low, middle, high))
        parts = halves if is_first(k) else 1
        per_group = parts * LANES // GROUPS
        count = rows * rows_n * cols * cols_n * per_group
        rows_out = []
        for part in range(parts):
            norm = (norm_first_ref[:, part * LANES:(part + 1) * LANES] if is_first(k) else norm_rest_ref[number(k) - 1]).astype(F32)
            mean = total[part:part + 1] / count
            square = total[parts + part:parts + part + 1] / count
            scale = lax.rsqrt(square - mean * mean + GN_EPS) * norm[0:1]
            shift = norm[1:2] - mean * scale
            rows_out.append((0.5 * scale, 0.5 * shift))
        return rows_out

    def activate_rows(k, s, scale_rows):
        for part, (scale, shift) in enumerate(scale_rows):
            for side, there in ((0, "up"), (1, "down")):
                for place in range(3):
                    seen = has[there] if place == 1 else both(there, "left" if place == 0 else "right")
                    act = half_silu(halo(k, s)[side, place, part] * scale + shift)
                    halo_act[side, part, place * cols:(place + 1) * cols, :] = jnp.where(seen, act, 0.0)

    def activate(k, s, scale_rows, c):
        z = z_in if is_first(k) else z_mid
        parts = len(scale_rows)
        for part, (scale, shift) in enumerate(scale_rows):
            ref = tile(k, s, c).at[part] if is_first(k) else tile(k, s, c)
            act = half_silu(ref[...].astype(F32) * scale + shift)
            if c in (0, cols + 1):
                act = jnp.where(has["left" if c == 0 else "right"], act, 0.0)
            at = cols - 1 + c
            above = jnp.concatenate([halo_act[0, part, at:at + 1, :], act[:-1]], axis=0)
            below = jnp.concatenate([act[1:], halo_act[1, part, at:at + 1, :]], axis=0)
            for dr, value in enumerate((above, act, below)):
                z[(c * 3 + dr) * parts + part] = value.astype(BF16)

    def wait_cols(k, s):
        for at, there in enumerate((has["right"], has["left"])):
            pl.when(there)(lambda at=at: col_copy(k, s, at).wait_recv())

    def layer(k, s):
        z = z_in if is_first(k) else z_mid
        scale_rows = scales(k, s)
        parts = len(scale_rows)
        depth = 3 * parts
        weights = (w_first[...] if is_first(k) else w_rest[number(k) - 1]).reshape(4 * depth * LANES, 2 * LANES)
        bias = bias_rows[number(k)]
        later = following(k)
        edge = edges(later, s)

        def pair(p, sums):
            lhs = jnp.concatenate([z[2 * p * depth + i] for i in range(4 * depth)], axis=1)
            acc = jnp.dot(lhs, weights, preferred_element_type=F32)
            sum_one, sum_two = sums
            for o in range(2):
                c = 2 * p + o
                value = acc[:, o * LANES:(o + 1) * LANES] + bias
                if k[1]:
                    value = value + short[s, c]
                rounded = value.astype(BF16)
                tile(later, s, c + 1)[...] = rounded
                value = rounded.astype(F32)
                if k[1]:
                    short[s, c] = value
                edge[0, 0, c:c + 1, :] = value[0:1]
                edge[1, 0, c:c + 1, :] = value[rows - 1:rows]
                value = value.reshape(rows // 8, 8, LANES)
                sum_one = sum_one + jnp.sum(value, axis=0)
                sum_two = sum_two + jnp.sum(value * value, axis=0)
            return sum_one, sum_two

        zero = jnp.zeros((8, LANES), F32)
        sums = (zero, zero)
        activate_rows(k, s, scale_rows)
        done = set()
        order = list(range(1, cols // 2 - 1)) + [0, cols // 2 - 1]
        for p in order:
            if p == 0 and is_first(k):
                for c in range(1, cols + 1):
                    if c not in done:
                        activate(k, s, scale_rows, c)
                        done.add(c)
                wait_cols(k, s)
            for c in range(2 * p, 2 * p + 4):
                if c not in done:
                    activate(k, s, scale_rows, c)
                    done.add(c)
            sums = pair(p, sums)
        target = message(later, s)
        for at, part in enumerate(sums):
            target[at:at + 1, :] = jnp.sum(part, axis=0, keepdims=True)
        send_stats(later, s)
        send_rows(later, s)
        send_cols(later, s)
        sent(k, s, first=True if is_first(k) else None)

    chunk = 16

    def load(s):
        pltpu.make_async_copy(act_hbm.at[s], raw.at[s], act_sem.at[s]).wait()

        def step(i, sums):
            at = pl.multiple_of(i * chunk, chunk)
            sums = list(sums)
            for part in range(halves):
                value = raw[s, pl.ds(at, chunk), :, part * LANES:(part + 1) * LANES].astype(F32)
                flat[s, part, pl.ds(pl.multiple_of(at * cols, chunk * cols), chunk * cols), :] = value.reshape(chunk * cols, LANES)
                sums[part] = sums[part] + jnp.sum(value, axis=0)
                sums[halves + part] = sums[halves + part] + jnp.sum(value * value, axis=0)
            return tuple(sums)

        zero = jnp.zeros((cols, LANES), F32)
        sums = lax.fori_loop(0, rows // chunk, step, (zero,) * (2 * halves))
        for at, part in enumerate(sums):
            msg_in[s, at:at + 1, :] = jnp.sum(part, axis=0, keepdims=True)
        for part in range(halves):
            edge_in[s, 0, part] = flat[s, part, 0:cols, :]
            edge_in[s, 1, part] = flat[s, part, (rows - 1) * cols:, :]

    def turn(s, c):
        for part in range(halves):
            map_in[s, c + 1, part] = flat[s, part, pl.ds(c, rows, stride=cols), :].astype(BF16)

    first = (0, 0)
    for s in range(samples):
        load(s)
    for s in range(samples):
        turn(s, 0)
        turn(s, cols - 1)
    pl.semaphore_wait(barrier, peers_n)
    send_stats(first, 0)
    for s in range(samples):
        send_rows(first, s)
        send_cols(first, s)

    for k in range(layers - 1):
        for o in range(2):
            for dc in range(3):
                pltpu.make_async_copy(w_rest_hbm.at[k, :, dc], w_rest.at[k, o + dc, :, :, pl.ds(o * LANES, LANES)], weight_sem.at[k + 1]).start()
    for src_dst, at in zip(small, range(len(small))):
        pltpu.make_async_copy(*src_dst, small_sem.at[at]).wait()
    row_id = lax.broadcasted_iota(jnp.int32, (LANES, LANES), 0)
    lane_id = lax.broadcasted_iota(jnp.int32, (LANES, LANES), 1)
    for ones, per_group in ((ones_in, in_ch // GROUPS), (ones_mid, LANES // GROUPS)):
        ones[...] = jnp.where(row_id // per_group == lane_id // per_group, 1.0, 0.0).astype(BF16)
    for dr in range(3):
        w_first[3, dr, :, 0:LANES] = jnp.zeros((in_ch, LANES), BF16)
        w_first[0, dr, :, LANES:] = jnp.zeros((in_ch, LANES), BF16)
    pltpu.make_async_copy(w_short_hbm, w_short, weight_sem.at[layers]).wait()
    for at in range(layers + 1):
        bias_rows[at] = bias_ref[at:at + 1].astype(F32)
    skip_bias = bias_rows[layers]
    def skip_product(s, _):
        for c in range(cols):
            if 0 < c < cols - 1:
                turn(s, c)
            both_halves = jnp.concatenate([map_in[s, c + 1, part] for part in range(halves)], axis=1)
            short[s, c] = jnp.dot(both_halves, w_short[...], preferred_element_type=F32) + skip_bias
        return 0

    lax.fori_loop(0, samples, skip_product, 0)

    def clear(k, _):
        for dr in range(3):
            w_rest[k, 3, dr, :, 0:LANES] = jnp.zeros((LANES, LANES), BF16)
            w_rest[k, 0, dr, :, LANES:] = jnp.zeros((LANES, LANES), BF16)
        return 0

    lax.fori_loop(0, layers - 1, clear, 0)

    col_id = lax.broadcasted_iota(jnp.int32, (cols, LANES), 0)

    def head_block(j, _):
        for dr in range(3):
            blocks = []
            for ch in range(3):
                block = jnp.zeros((cols, LANES), F32)
                for dc in range(3):
                    block = jnp.where(col_id == j - dc, w_out_ref[dr, dc, ch:ch + 1, :].astype(F32), block)
                blocks.append(block)
            blocks.append(jnp.zeros((cols, LANES), F32))
            w_head[:, pl.ds(pl.multiple_of((j * 3 + dr) * LANES, LANES), LANES)] = jnp.concatenate(blocks, axis=0).astype(BF16)
        return 0

    lax.fori_loop(0, cols + 2, head_block, 0)

    def both_samples(k):
        if not is_first(k):
            at = number(k) - 1
            pltpu.make_async_copy(w_rest.at[at, 0:3], w_rest.at[at, 0:3], weight_sem.at[at + 1]).wait()
        lax.fori_loop(0, samples, lambda s, _: (layer(k, s), 0)[1], 0)

    pltpu.make_async_copy(w_first.at[0:3], w_first.at[0:3], weight_sem.at[0]).wait()
    pltpu.make_async_copy(got_in, got_in, stat_recv.at[0, 0]).wait()
    both_samples(first)
    pltpu.make_async_copy(got_in, got_in, stat_send.at[0, 0]).wait()
    both_samples((0, 1))

    def block(i, _):
        both_samples((i, 0))
        both_samples((i, 1))
        return 0

    lax.fori_loop(1, layers // 2, block, 0)
    last = (layers // 2, 0)

    def head(s, _):
        scale_rows = scales(last, s)
        activate_rows(last, s, scale_rows)

        def product(blocks):
            acts = jnp.concatenate([z_mid[i] for i in blocks], axis=1)
            weights = w_head[:, blocks[0] * LANES:(blocks[-1] + 1) * LANES]
            return lax.dot_general(weights, acts, (((1,), (1,)), ((), ())), preferred_element_type=F32)

        for c in range(cols + 2):
            activate(last, s, scale_rows, c)
        rgb = product(range(3 * (cols + 2)))
        for ch in range(3):
            out_ref[s, ch] = rgb[ch * cols:(ch + 1) * cols] + bias_out_ref[:, ch:ch + 1].astype(F32)
        sent(last, s)
        return 0

    lax.fori_loop(0, samples, head, 0)


def solution(mesh):
    rows_n = mesh.shape["sy"]
    cols_n = mesh.shape["sx"]
    tile_spec = P("dp", "sy", "sx", None)
    replicated = P()

    def local_decode(act_in, norm_first, w_first, w_short, norm_rest, w_rest, bias_rest, w_out, bias_out):
        samples, rows, cols, in_ch = act_in.shape
        halves = in_ch // LANES
        layers = w_rest.shape[0] + 1
        peers_n = rows_n * cols_n - 1
        in_hbm = pl.BlockSpec(memory_space=pltpu.HBM)
        in_vmem = pl.BlockSpec(memory_space=pltpu.VMEM)
        image = pl.pallas_call(
            functools.partial(decode_kernel, rows_n, cols_n),
            out_shape=jax.ShapeDtypeStruct((samples, 3, cols, rows), F32),
            in_specs=[in_hbm] * 9,
            out_specs=in_vmem,
            scratch_shapes=[
                pltpu.VMEM((samples, rows, cols, in_ch), BF16),
                pltpu.VMEM((samples, halves, rows * cols, LANES), F32),
                pltpu.VMEM((samples, cols + 2, halves, rows, LANES), BF16),
                pltpu.VMEM(((layers + 1) // 2, samples, cols + 2, rows, LANES), BF16),
                pltpu.VMEM(((layers + 1) // 2, samples, cols + 2, rows, LANES), BF16),
                pltpu.VMEM(((cols + 2) * 3 * halves, rows, LANES), BF16),
                pltpu.VMEM(((cols + 2) * 3, rows, LANES), BF16),
                pltpu.VMEM((samples, cols, rows, LANES), F32),
                pltpu.VMEM((4, 3, in_ch, 2 * LANES), BF16),
                pltpu.VMEM((in_ch, LANES), BF16),
                pltpu.VMEM((layers - 1, 4, 3, LANES, 2 * LANES), BF16),
                pltpu.VMEM((4 * cols, (cols + 2) * 3 * LANES), BF16),
                pltpu.VMEM((LANES, LANES), BF16),
                pltpu.VMEM((LANES, LANES), BF16),
                pltpu.VMEM(norm_first.shape, BF16),
                pltpu.VMEM(norm_rest.shape, BF16),
                pltpu.VMEM(bias_rest.shape, BF16),
                pltpu.VMEM((bias_rest.shape[0], 1, LANES), F32),
                pltpu.VMEM((3, 3, 3, LANES), BF16),
                pltpu.VMEM((1, 3), BF16),
                pltpu.VMEM((samples, 2 * halves, LANES), F32),
                pltpu.VMEM((layers, samples, 2, LANES), F32),
                pltpu.VMEM((peers_n, samples, 2 * halves, LANES), F32),
                pltpu.VMEM((layers, samples, peers_n, 2, LANES), F32),
                pltpu.VMEM((samples, 2, halves, cols, LANES), F32),
                pltpu.VMEM((layers, samples, 2, 1, cols, LANES), F32),
                pltpu.VMEM((samples, 2, 3, halves, cols, LANES), F32),
                pltpu.VMEM((layers, samples, 2, 3, 1, cols, LANES), F32),
                pltpu.VMEM((2, halves, 3 * cols, LANES), F32),
                pltpu.SemaphoreType.DMA((samples,)),
                pltpu.SemaphoreType.DMA((layers + 1,)),
                pltpu.SemaphoreType.DMA((5,)),
                pltpu.SemaphoreType.DMA((layers + 1, samples)),
                pltpu.SemaphoreType.DMA((layers + 1, samples)),
                pltpu.SemaphoreType.DMA((layers + 1, samples, 8)),
                pltpu.SemaphoreType.DMA((layers + 1, samples, 8)),
            ],
            compiler_params=pltpu.CompilerParams(collective_id=0, has_side_effects=True, vmem_limit_bytes=36 * 1024 * 1024),
            name="decode",
        )(*(pltpu.with_memory_space_constraint(x, pltpu.HBM) for x in (act_in, w_first, w_short, w_rest, norm_first, norm_rest, bias_rest, jnp.transpose(w_out, (0, 1, 3, 2)), bias_out.reshape(1, 3))))
        return jnp.transpose(image, (0, 3, 2, 1))

    return jax.shard_map(local_decode, mesh=mesh, in_specs=(tile_spec,) + (replicated,) * 8, out_specs=tile_spec, check_vma=False)
```

```python
import functools

import jax
import jax.numpy as jnp
from jax import lax
from jax.experimental import pallas as pl
from jax.experimental.pallas import tpu as pltpu
from jax.sharding import PartitionSpec as P

GROUPS = 32
GN_EPS = 1e-6
LANES = 128
MESH = pl.DeviceIdType.MESH
F32 = jnp.float32
BF16 = jnp.bfloat16


def half_silu(half):
    return half + half * jnp.tanh(half)


def decode_kernel(rows_n, cols_n, act_hbm, w_first_hbm, w_short_hbm, w_rest_hbm, norm_first_hbm, norm_rest_hbm, bias_hbm, w_out_hbm, bias_out_hbm, out_ref,
                  raw, flat, map_in, mid_maps, hidden_maps, z_in, z_mid, short, w_first, w_short, w_rest, w_head, z_edge, ones_in, ones_mid,
                  norm_first_ref, norm_rest_ref, bias_ref, bias_rows, w_out_ref, bias_out_ref,
                  msg_in, msg_mid, got_in, got_mid, edge_in, edge_mid, halo_in, halo_mid, halo_act,
                  act_sem, weight_sem, small_sem, stat_recv, stat_send, halo_recv, halo_send):
    samples, rows, cols, in_ch = raw.shape
    halves = in_ch // LANES
    layers = w_rest.shape[0] + 1
    peers_n = rows_n * cols_n - 1
    sx = lax.axis_index("sx")
    sy = lax.axis_index("sy")
    core = lax.rem(sy, 2)
    chip = sy // 2
    chips_n = rows_n // 2

    def ring(offset, size):
        return min(offset, size - offset)

    offsets = [(dx, dy, dc) for dx in range(cols_n) for dy in range(chips_n) for dc in range(2) if (dx, dy, dc) != (0, 0, 0)]
    offsets.sort(key=lambda o: (-ring(o[0], cols_n) - ring(o[1], chips_n), o[2]))

    def peer(offset):
        dx, dy, dc = offset
        return {"sx": lax.rem(sx + dx, cols_n), "sy": lax.rem(chip + dy, chips_n) * 2 + (1 - core if dc else core)}

    barrier = pltpu.get_barrier_semaphore()
    for offset in offsets:
        pl.semaphore_signal(barrier, inc=1, device_id=peer(offset), device_id_type=MESH)

    for s in range(samples):
        pltpu.make_async_copy(act_hbm.at[s], raw.at[s], act_sem.at[s]).start()
    small = [(norm_first_hbm, norm_first_ref), (norm_rest_hbm, norm_rest_ref), (bias_hbm, bias_ref), (w_out_hbm, w_out_ref), (bias_out_hbm, bias_out_ref)]
    for at, (src, dst) in enumerate(small):
        pltpu.make_async_copy(src, dst, small_sem.at[at]).start()
    pltpu.make_async_copy(w_short_hbm, w_short, weight_sem.at[layers]).start()
    for o in range(2):
        for dc in range(3):
            pltpu.make_async_copy(w_first_hbm.at[:, dc], w_first.at[o + dc, :, :, pl.ds(o * LANES, LANES)], weight_sem.at[0]).start()

    has = {"up": sy > 0, "down": sy < rows_n - 1, "left": sx > 0, "right": sx < cols_n - 1}

    def both(one, two):
        return jnp.logical_and(has[one], has[two])

    row_moves = [
        (1, 1, 0, {"sy": sy - 1}, has["up"], has["down"]),
        (0, 1, 1, {"sy": sy + 1}, has["down"], has["up"]),
        (1, 2, 0, {"sx": sx - 1, "sy": sy - 1}, both("up", "left"), both("down", "right")),
        (1, 0, 0, {"sx": sx + 1, "sy": sy - 1}, both("up", "right"), both("down", "left")),
        (0, 2, 1, {"sx": sx - 1, "sy": sy + 1}, both("down", "left"), both("up", "right")),
        (0, 0, 1, {"sx": sx + 1, "sy": sy + 1}, both("down", "right"), both("up", "left")),
    ]

    def is_first(k):
        return k[1] == 0 and isinstance(k[0], int) and k[0] == 0

    def number(k):
        return 2 * k[0] + k[1]

    def following(k):
        return (k[0], 1) if k[1] == 0 else (k[0] + 1, 0)

    def tile(k, s, c):
        if is_first(k):
            return map_in.at[s, c]
        return mid_maps.at[k[0], s, c] if k[1] else hidden_maps.at[k[0] - 1, s, c]

    def edges(k, s):
        return edge_in.at[s] if is_first(k) else edge_mid.at[number(k) - 1, s]

    def halo(k, s):
        return halo_in.at[s] if is_first(k) else halo_mid.at[number(k) - 1, s]

    def message(k, s):
        return msg_in if is_first(k) else msg_mid.at[number(k) - 1, s]

    def received(k, s):
        return got_in if is_first(k) else got_mid.at[number(k) - 1, s]

    def col_copy(k, s, at):
        src, dst, to = ((1, cols + 1, {"sx": sx - 1}), (cols, 0, {"sx": sx + 1}))[at]
        return pltpu.make_async_remote_copy(tile(k, s, src), tile(k, s, dst), halo_send.at[number(k), s, at], halo_recv.at[number(k), s, at], device_id=to, device_id_type=MESH)

    def row_copy(k, s, at):
        side, place, edge, to, _, _ = row_moves[at]
        return pltpu.make_async_remote_copy(edges(k, s).at[edge], halo(k, s).at[side, place], halo_send.at[number(k), s, 2 + at], halo_recv.at[number(k), s, 2 + at], device_id=to, device_id_type=MESH)

    def send_cols(k, s):
        for at, there in enumerate((has["left"], has["right"])):
            pl.when(there)(lambda at=at: col_copy(k, s, at).start())

    def send_rows(k, s):
        for at, move in enumerate(row_moves):
            pl.when(move[4])(lambda at=at: row_copy(k, s, at).start())

    def send_stats(k, s):
        for slot, offset in enumerate(offsets):
            pltpu.make_async_remote_copy(message(k, s), received(k, s).at[slot], stat_send.at[number(k), s], stat_recv.at[number(k), s], device_id=peer(offset), device_id_type=MESH).start()

    def sent(k, s, first=None):
        if first is None:
            pltpu.make_async_copy(received(k, s), received(k, s), stat_send.at[number(k), s]).wait()
        for at, there in enumerate((has["left"], has["right"])):
            pl.when(there)(lambda at=at: col_copy(k, s, at).wait_send())
        for at, move in enumerate(row_moves):
            pl.when(move[4])(lambda at=at: row_copy(k, s, at).wait_send())

    def wait_rows(k, s):
        for at, move in enumerate(row_moves):
            pl.when(move[5])(lambda at=at: row_copy(k, s, at).wait_recv())

    def scales(k, s):
        wait_rows(k, s)
        if is_first(k):
            total = msg_in[s] + jnp.sum(got_in[:, s], axis=0)
        else:
            wait_cols(k, s)
            pltpu.make_async_copy(received(k, s), received(k, s), stat_recv.at[number(k), s]).wait()
            total = message(k, s)[...] + jnp.sum(received(k, s)[...], axis=0)
        ones = ones_in if is_first(k) else ones_mid
        high = total.astype(BF16)
        rest = total - high.astype(F32)
        middle = rest.astype(BF16)
        low = (rest - middle.astype(F32)).astype(BF16)
        total = sum(jnp.dot(piece, ones[...], preferred_element_type=F32) for piece in (low, middle, high))
        parts = halves if is_first(k) else 1
        per_group = parts * LANES // GROUPS
        count = rows * rows_n * cols * cols_n * per_group
        rows_out = []
        for part in range(parts):
            norm = (norm_first_ref[:, part * LANES:(part + 1) * LANES] if is_first(k) else norm_rest_ref[number(k) - 1]).astype(F32)
            mean = total[part:part + 1] * (1.0 / count)
            square = total[parts + part:parts + part + 1] * (1.0 / count)
            scale = lax.rsqrt(square - mean * mean + GN_EPS) * norm[0:1]
            shift = norm[1:2] - mean * scale
            rows_out.append((0.5 * scale, 0.5 * shift))
        return rows_out

    def activate_rows(k, s, scale_rows):
        for part, (scale, shift) in enumerate(scale_rows):
            for side, there in ((0, "up"), (1, "down")):
                for place in range(3):
                    seen = has[there] if place == 1 else both(there, "left" if place == 0 else "right")
                    act = half_silu(halo(k, s)[side, place, part] * scale + shift)
                    halo_act[side, part, place * cols:(place + 1) * cols, :] = jnp.where(seen, act, 0.0)

    def activate(k, s, scale_rows, c):
        z = z_in if is_first(k) else z_mid
        parts = len(scale_rows)
        for part, (scale, shift) in enumerate(scale_rows):
            ref = tile(k, s, c).at[part] if is_first(k) else tile(k, s, c)
            act = half_silu(ref[...].astype(F32) * scale + shift)
            if c in (0, cols + 1):
                act = jnp.where(has["left" if c == 0 else "right"], act, 0.0)
            at = cols - 1 + c
            above = jnp.concatenate([halo_act[0, part, at:at + 1, :], act[:-1]], axis=0)
            below = jnp.concatenate([act[1:], halo_act[1, part, at:at + 1, :]], axis=0)
            for dr, value in enumerate((above, act, below)):
                z[(c * 3 + dr) * parts + part] = value.astype(BF16)

    def wait_cols(k, s):
        for at, there in enumerate((has["right"], has["left"])):
            pl.when(there)(lambda at=at: col_copy(k, s, at).wait_recv())

    def layer(k, s):
        z = z_in if is_first(k) else z_mid
        scale_rows = scales(k, s)
        parts = len(scale_rows)
        depth = 3 * parts
        weights = (w_first[...] if is_first(k) else w_rest[number(k) - 1]).reshape(4 * depth * LANES, 2 * LANES)
        bias = bias_rows[number(k)]
        later = following(k)
        edge = edges(later, s)

        def pair(p, sums):
            lhs = jnp.concatenate([z[2 * p * depth + i] for i in range(4 * depth)], axis=1)
            acc = jnp.dot(lhs, weights, preferred_element_type=F32)
            sum_one, sum_two = sums
            for o in range(2):
                c = 2 * p + o
                value = acc[:, o * LANES:(o + 1) * LANES] + bias
                if k[1]:
                    value = value + short[s, c]
                rounded = value.astype(BF16)
                tile(later, s, c + 1)[...] = rounded
                value = rounded.astype(F32)
                if k[1]:
                    short[s, c] = value
                edge[0, 0, c:c + 1, :] = value[0:1]
                edge[1, 0, c:c + 1, :] = value[rows - 1:rows]
                value = value.reshape(rows // 8, 8, LANES)
                sum_one = sum_one + jnp.sum(value, axis=0)
                sum_two = sum_two + jnp.sum(value * value, axis=0)
            return sum_one, sum_two

        zero = jnp.zeros((8, LANES), F32)
        sums = (zero, zero)
        activate_rows(k, s, scale_rows)
        done = set()
        order = list(range(1, cols // 2 - 1)) + [0, cols // 2 - 1]
        for p in order:
            if p == 0 and is_first(k):
                for c in range(1, cols + 1):
                    if c not in done:
                        activate(k, s, scale_rows, c)
                        done.add(c)
                wait_cols(k, s)
            for c in range(2 * p, 2 * p + 4):
                if c not in done:
                    activate(k, s, scale_rows, c)
                    done.add(c)
            sums = pair(p, sums)
        target = message(later, s)
        for at, part in enumerate(sums):
            target[at:at + 1, :] = jnp.sum(part, axis=0, keepdims=True)
        send_stats(later, s)
        send_rows(later, s)
        send_cols(later, s)
        sent(k, s, first=True if is_first(k) else None)

    chunk = 16

    def load(s):
        pltpu.make_async_copy(act_hbm.at[s], raw.at[s], act_sem.at[s]).wait()

        def step(i, sums):
            at = pl.multiple_of(i * chunk, chunk)
            sums = list(sums)
            for part in range(halves):
                value = raw[s, pl.ds(at, chunk), :, part * LANES:(part + 1) * LANES].astype(F32)
                flat[s, part, pl.ds(pl.multiple_of(at * cols, chunk * cols), chunk * cols), :] = value.reshape(chunk * cols, LANES)
                sums[part] = sums[part] + jnp.sum(value, axis=0)
                sums[halves + part] = sums[halves + part] + jnp.sum(value * value, axis=0)
            return tuple(sums)

        zero = jnp.zeros((cols, LANES), F32)
        sums = lax.fori_loop(0, rows // chunk, step, (zero,) * (2 * halves))
        for at, part in enumerate(sums):
            msg_in[s, at:at + 1, :] = jnp.sum(part, axis=0, keepdims=True)
        for part in range(halves):
            edge_in[s, 0, part] = flat[s, part, 0:cols, :]
            edge_in[s, 1, part] = flat[s, part, (rows - 1) * cols:, :]

    def turn(s, c):
        for part in range(halves):
            map_in[s, c + 1, part] = flat[s, part, pl.ds(c, rows, stride=cols), :].astype(BF16)

    first = (0, 0)
    for s in range(samples):
        load(s)
    for s in range(samples):
        turn(s, 0)
        turn(s, cols - 1)
    pl.semaphore_wait(barrier, peers_n)
    send_stats(first, 0)
    for s in range(samples):
        send_rows(first, s)
        send_cols(first, s)

    for k in range(layers - 1):
        for o in range(2):
            for dc in range(3):
                pltpu.make_async_copy(w_rest_hbm.at[k, :, dc], w_rest.at[k, o + dc, :, :, pl.ds(o * LANES, LANES)], weight_sem.at[k + 1]).start()
    for src_dst, at in zip(small, range(len(small))):
        pltpu.make_async_copy(*src_dst, small_sem.at[at]).wait()
    row_id = lax.broadcasted_iota(jnp.int32, (LANES, LANES), 0)
    lane_id = lax.broadcasted_iota(jnp.int32, (LANES, LANES), 1)
    for ones, per_group in ((ones_in, in_ch // GROUPS), (ones_mid, LANES // GROUPS)):
        ones[...] = jnp.where(row_id // per_group == lane_id // per_group, 1.0, 0.0).astype(BF16)
    for dr in range(3):
        w_first[3, dr, :, 0:LANES] = jnp.zeros((in_ch, LANES), BF16)
        w_first[0, dr, :, LANES:] = jnp.zeros((in_ch, LANES), BF16)
    pltpu.make_async_copy(w_short_hbm, w_short, weight_sem.at[layers]).wait()
    for at in range(layers + 1):
        bias_rows[at] = bias_ref[at:at + 1].astype(F32)
    skip_bias = bias_rows[layers]
    def skip_product(s, _):
        for c in range(cols):
            if 0 < c < cols - 1:
                turn(s, c)
            both_halves = jnp.concatenate([map_in[s, c + 1, part] for part in range(halves)], axis=1)
            short[s, c] = jnp.dot(both_halves, w_short[...], preferred_element_type=F32) + skip_bias
        return 0

    lax.fori_loop(0, samples, skip_product, 0)

    def clear(k, _):
        for dr in range(3):
            w_rest[k, 3, dr, :, 0:LANES] = jnp.zeros((LANES, LANES), BF16)
            w_rest[k, 0, dr, :, LANES:] = jnp.zeros((LANES, LANES), BF16)
        return 0

    lax.fori_loop(0, layers - 1, clear, 0)

    col_id = lax.broadcasted_iota(jnp.int32, (cols, LANES), 0)

    def head_block(j, _):
        blocks = []
        for dr in range(3):
            for ch in range(3):
                block = jnp.zeros((cols, LANES), F32)
                for dc in range(3):
                    block = jnp.where(col_id == j - dc, w_out_ref[dr, dc, ch:ch + 1, :].astype(F32), block)
                blocks.append(block)
        blocks.append(jnp.zeros((cols, LANES), F32))
        w_head[:, pl.ds(pl.multiple_of(j * LANES, LANES), LANES)] = jnp.concatenate(blocks, axis=0).astype(BF16)
        return 0

    lax.fori_loop(0, cols + 2, head_block, 0)

    def both_samples(k):
        if not is_first(k):
            at = number(k) - 1
            pltpu.make_async_copy(w_rest.at[at, 0:3], w_rest.at[at, 0:3], weight_sem.at[at + 1]).wait()
        lax.fori_loop(0, samples, lambda s, _: (layer(k, s), 0)[1], 0)

    pltpu.make_async_copy(w_first.at[0:3], w_first.at[0:3], weight_sem.at[0]).wait()
    pltpu.make_async_copy(got_in, got_in, stat_recv.at[0, 0]).wait()
    both_samples(first)
    pltpu.make_async_copy(got_in, got_in, stat_send.at[0, 0]).wait()
    both_samples((0, 1))

    def block(i, _):
        both_samples((i, 0))
        both_samples((i, 1))
        return 0

    lax.fori_loop(1, layers // 2, block, 0)
    last = (layers // 2, 0)

    def head(s, _):
        scale_rows = scales(last, s)
        activate_rows(last, s, scale_rows)

        scale, shift = scale_rows[0]
        for c in range(cols + 2):
            act = half_silu(tile(last, s, c)[...].astype(F32) * scale + shift)
            if c in (0, cols + 1):
                act = jnp.where(has["left" if c == 0 else "right"], act, 0.0)
            z_mid[c] = act.astype(BF16)
            at = cols - 1 + c
            ends = [halo_act[side, 0, at:at + 1, :] for side in range(2)] + [jnp.zeros((14, LANES), F32)]
            z_edge[c] = jnp.concatenate(ends, axis=0).astype(BF16)

        def product(ref):
            acts = jnp.concatenate([ref[c] for c in range(cols + 2)], axis=1)
            return lax.dot_general(w_head[...], acts, (((1,), (1,)), ((), ())), preferred_element_type=F32)

        taps = product(z_mid)
        ends = product(z_edge)
        part = 3 * cols
        above = jnp.concatenate([ends[:part, 0:1], taps[:part, :-1]], axis=1)
        below = jnp.concatenate([taps[2 * part:3 * part, 1:], ends[2 * part:3 * part, 1:2]], axis=1)
        rgb = above + taps[part:2 * part] + below
        for ch in range(3):
            out_ref[s, ch] = rgb[ch * cols:(ch + 1) * cols] + bias_out_ref[:, ch:ch + 1].astype(F32)
        sent(last, s)
        return 0

    lax.fori_loop(0, samples, head, 0)


def solution(mesh):
    rows_n = mesh.shape["sy"]
    cols_n = mesh.shape["sx"]
    tile_spec = P("dp", "sy", "sx", None)
    replicated = P()

    def local_decode(act_in, norm_first, w_first, w_short, norm_rest, w_rest, bias_rest, w_out, bias_out):
        samples, rows, cols, in_ch = act_in.shape
        halves = in_ch // LANES
        layers = w_rest.shape[0] + 1
        peers_n = rows_n * cols_n - 1
        in_hbm = pl.BlockSpec(memory_space=pltpu.HBM)
        in_vmem = pl.BlockSpec(memory_space=pltpu.VMEM)
        image = pl.pallas_call(
            functools.partial(decode_kernel, rows_n, cols_n),
            out_shape=jax.ShapeDtypeStruct((samples, 3, cols, rows), F32),
            in_specs=[in_hbm] * 9,
            out_specs=in_vmem,
            scratch_shapes=[
                pltpu.VMEM((samples, rows, cols, in_ch), BF16),
                pltpu.VMEM((samples, halves, rows * cols, LANES), F32),
                pltpu.VMEM((samples, cols + 2, halves, rows, LANES), BF16),
                pltpu.VMEM(((layers + 1) // 2, samples, cols + 2, rows, LANES), BF16),
                pltpu.VMEM(((layers + 1) // 2, samples, cols + 2, rows, LANES), BF16),
                pltpu.VMEM(((cols + 2) * 3 * halves, rows, LANES), BF16),
                pltpu.VMEM(((cols + 2) * 3, rows, LANES), BF16),
                pltpu.VMEM((samples, cols, rows, LANES), F32),
                pltpu.VMEM((4, 3, in_ch, 2 * LANES), BF16),
                pltpu.VMEM((in_ch, LANES), BF16),
                pltpu.VMEM((layers - 1, 4, 3, LANES, 2 * LANES), BF16),
                pltpu.VMEM((10 * cols, (cols + 2) * LANES), BF16),
                pltpu.VMEM((cols + 2, 16, LANES), BF16),
                pltpu.VMEM((LANES, LANES), BF16),
                pltpu.VMEM((LANES, LANES), BF16),
                pltpu.VMEM(norm_first.shape, BF16),
                pltpu.VMEM(norm_rest.shape, BF16),
                pltpu.VMEM(bias_rest.shape, BF16),
                pltpu.VMEM((bias_rest.shape[0], 1, LANES), F32),
                pltpu.VMEM((3, 3, 3, LANES), BF16),
                pltpu.VMEM((1, 3), BF16),
                pltpu.VMEM((samples, 2 * halves, LANES), F32),
                pltpu.VMEM((layers, samples, 2, LANES), F32),
                pltpu.VMEM((peers_n, samples, 2 * halves, LANES), F32),
                pltpu.VMEM((layers, samples, peers_n, 2, LANES), F32),
                pltpu.VMEM((samples, 2, halves, cols, LANES), F32),
                pltpu.VMEM((layers, samples, 2, 1, cols, LANES), F32),
                pltpu.VMEM((samples, 2, 3, halves, cols, LANES), F32),
                pltpu.VMEM((layers, samples, 2, 3, 1, cols, LANES), F32),
                pltpu.VMEM((2, halves, 3 * cols, LANES), F32),
                pltpu.SemaphoreType.DMA((samples,)),
                pltpu.SemaphoreType.DMA((layers + 1,)),
                pltpu.SemaphoreType.DMA((5,)),
                pltpu.SemaphoreType.DMA((layers + 1, samples)),
                pltpu.SemaphoreType.DMA((layers + 1, samples)),
                pltpu.SemaphoreType.DMA((layers + 1, samples, 8)),
                pltpu.SemaphoreType.DMA((layers + 1, samples, 8)),
            ],
            compiler_params=pltpu.CompilerParams(collective_id=0, has_side_effects=True, vmem_limit_bytes=36 * 1024 * 1024),
            name="decode",
        )(*(pltpu.with_memory_space_constraint(x, pltpu.HBM) for x in (act_in, w_first, w_short, w_rest, norm_first, norm_rest, bias_rest, jnp.transpose(w_out, (0, 1, 3, 2)), bias_out.reshape(1, 3))))
        return jnp.transpose(image, (0, 3, 2, 1))

    return jax.shard_map(local_decode, mesh=mesh, in_specs=(tile_spec,) + (replicated,) * 8, out_specs=tile_spec, check_vma=False)
```

```python
import functools

import jax
import jax.numpy as jnp
from jax import lax
from jax.experimental import pallas as pl
from jax.experimental.pallas import tpu as pltpu
from jax.sharding import PartitionSpec as P

GROUPS = 32
GN_EPS = 1e-6
LANES = 128
MESH = pl.DeviceIdType.MESH
F32 = jnp.float32
BF16 = jnp.bfloat16


def half_silu(half):
    return half + half * jnp.tanh(half)


def decode_kernel(rows_n, cols_n, act_hbm, w_first_hbm, w_short_hbm, w_rest_hbm, norm_first_hbm, norm_rest_hbm, bias_hbm, w_out_hbm, bias_out_hbm, out_ref,
                  raw, flat, map_in, mid_maps, hidden_maps, z_in, z_mid, short, w_first, w_short, w_rest, w_head, z_edge, ones_in, ones_mid,
                  norm_first_ref, norm_rest_ref, bias_ref, bias_rows, w_out_ref, bias_out_ref,
                  msg_in, msg_mid, got_in, got_mid, edge_in, edge_mid, halo_in, halo_mid, halo_act,
                  act_sem, weight_sem, small_sem, stat_recv, stat_send, halo_recv, halo_send):
    samples, rows, cols, in_ch = raw.shape
    halves = in_ch // LANES
    layers = w_rest.shape[0] + 1
    peers_n = rows_n * cols_n - 1
    sx = lax.axis_index("sx")
    sy = lax.axis_index("sy")
    core = lax.rem(sy, 2)
    chip = sy // 2
    chips_n = rows_n // 2

    def ring(offset, size):
        return min(offset, size - offset)

    offsets = [(dx, dy, dc) for dx in range(cols_n) for dy in range(chips_n) for dc in range(2) if (dx, dy, dc) != (0, 0, 0)]
    offsets.sort(key=lambda o: (-ring(o[0], cols_n) - ring(o[1], chips_n), o[2]))

    def peer(offset):
        dx, dy, dc = offset
        return {"sx": lax.rem(sx + dx, cols_n), "sy": lax.rem(chip + dy, chips_n) * 2 + (1 - core if dc else core)}

    barrier = pltpu.get_barrier_semaphore()
    for offset in offsets:
        pl.semaphore_signal(barrier, inc=1, device_id=peer(offset), device_id_type=MESH)

    for s in range(samples):
        pltpu.make_async_copy(act_hbm.at[s], raw.at[s], act_sem.at[s]).start()
    small = [(norm_first_hbm, norm_first_ref), (norm_rest_hbm, norm_rest_ref), (bias_hbm, bias_ref), (w_out_hbm, w_out_ref), (bias_out_hbm, bias_out_ref)]
    for at, (src, dst) in enumerate(small):
        pltpu.make_async_copy(src, dst, small_sem.at[at]).start()
    pltpu.make_async_copy(w_short_hbm, w_short, weight_sem.at[layers]).start()
    for o in range(2):
        for dc in range(3):
            pltpu.make_async_copy(w_first_hbm.at[:, dc], w_first.at[o + dc, :, :, pl.ds(o * LANES, LANES)], weight_sem.at[0]).start()

    has = {"up": sy > 0, "down": sy < rows_n - 1, "left": sx > 0, "right": sx < cols_n - 1}

    def both(one, two):
        return jnp.logical_and(has[one], has[two])

    row_moves = [
        (1, 1, 0, {"sy": sy - 1}, has["up"], has["down"]),
        (0, 1, 1, {"sy": sy + 1}, has["down"], has["up"]),
        (1, 2, 0, {"sx": sx - 1, "sy": sy - 1}, both("up", "left"), both("down", "right")),
        (1, 0, 0, {"sx": sx + 1, "sy": sy - 1}, both("up", "right"), both("down", "left")),
        (0, 2, 1, {"sx": sx - 1, "sy": sy + 1}, both("down", "left"), both("up", "right")),
        (0, 0, 1, {"sx": sx + 1, "sy": sy + 1}, both("down", "right"), both("up", "left")),
    ]

    def is_first(k):
        return k[1] == 0 and isinstance(k[0], int) and k[0] == 0

    def number(k):
        return 2 * k[0] + k[1]

    def following(k):
        return (k[0], 1) if k[1] == 0 else (k[0] + 1, 0)

    def tile(k, s, c):
        if is_first(k):
            return map_in.at[s, c]
        return mid_maps.at[k[0], s, c] if k[1] else hidden_maps.at[k[0] - 1, s, c]

    def edges(k, s):
        return edge_in.at[s] if is_first(k) else edge_mid.at[number(k) - 1, s]

    def halo(k, s):
        return halo_in.at[s] if is_first(k) else halo_mid.at[number(k) - 1, s]

    def message(k, s):
        return msg_in if is_first(k) else msg_mid.at[number(k) - 1, s]

    def received(k, s):
        return got_in if is_first(k) else got_mid.at[number(k) - 1, s]

    def col_copy(k, s, at):
        src, dst, to = ((1, cols + 1, {"sx": sx - 1}), (cols, 0, {"sx": sx + 1}))[at]
        return pltpu.make_async_remote_copy(tile(k, s, src), tile(k, s, dst), halo_send.at[number(k), s, at], halo_recv.at[number(k), s, at], device_id=to, device_id_type=MESH)

    def row_copy(k, s, at):
        side, place, edge, to, _, _ = row_moves[at]
        return pltpu.make_async_remote_copy(edges(k, s).at[edge], halo(k, s).at[side, place], halo_send.at[number(k), s, 2 + at], halo_recv.at[number(k), s, 2 + at], device_id=to, device_id_type=MESH)

    def send_cols(k, s):
        for at, there in enumerate((has["left"], has["right"])):
            pl.when(there)(lambda at=at: col_copy(k, s, at).start())

    def send_rows(k, s):
        for at, move in enumerate(row_moves):
            pl.when(move[4])(lambda at=at: row_copy(k, s, at).start())

    def send_stats(k, s):
        for slot, offset in enumerate(offsets):
            pltpu.make_async_remote_copy(message(k, s), received(k, s).at[slot], stat_send.at[number(k), s], stat_recv.at[number(k), s], device_id=peer(offset), device_id_type=MESH).start()

    def sent(k, s, first=None):
        if first is None:
            pltpu.make_async_copy(received(k, s), received(k, s), stat_send.at[number(k), s]).wait()
        for at, there in enumerate((has["left"], has["right"])):
            pl.when(there)(lambda at=at: col_copy(k, s, at).wait_send())
        for at, move in enumerate(row_moves):
            pl.when(move[4])(lambda at=at: row_copy(k, s, at).wait_send())

    def wait_rows(k, s):
        for at, move in enumerate(row_moves):
            pl.when(move[5])(lambda at=at: row_copy(k, s, at).wait_recv())

    def scales(k, s):
        wait_rows(k, s)
        if is_first(k):
            total = msg_in[s] + jnp.sum(got_in[:, s], axis=0)
        else:
            wait_cols(k, s)
            pltpu.make_async_copy(received(k, s), received(k, s), stat_recv.at[number(k), s]).wait()
            total = message(k, s)[...] + jnp.sum(received(k, s)[...], axis=0)
        ones = ones_in if is_first(k) else ones_mid
        high = total.astype(BF16)
        rest = total - high.astype(F32)
        middle = rest.astype(BF16)
        low = (rest - middle.astype(F32)).astype(BF16)
        total = sum(jnp.dot(piece, ones[...], preferred_element_type=F32) for piece in (low, middle, high))
        parts = halves if is_first(k) else 1
        per_group = parts * LANES // GROUPS
        count = rows * rows_n * cols * cols_n * per_group
        rows_out = []
        for part in range(parts):
            norm = (norm_first_ref[:, part * LANES:(part + 1) * LANES] if is_first(k) else norm_rest_ref[number(k) - 1]).astype(F32)
            mean = total[part:part + 1] * (1.0 / count)
            square = total[parts + part:parts + part + 1] * (1.0 / count)
            scale = lax.rsqrt(square - mean * mean + GN_EPS) * norm[0:1]
            shift = norm[1:2] - mean * scale
            rows_out.append((0.5 * scale, 0.5 * shift))
        return rows_out

    def activate_rows(k, s, scale_rows):
        for part, (scale, shift) in enumerate(scale_rows):
            for side, there in ((0, "up"), (1, "down")):
                for place in range(3):
                    seen = has[there] if place == 1 else both(there, "left" if place == 0 else "right")
                    act = half_silu(halo(k, s)[side, place, part] * scale + shift)
                    halo_act[side, part, place * cols:(place + 1) * cols, :] = jnp.where(seen, act, 0.0)

    def activate(k, s, scale_rows, c):
        z = z_in if is_first(k) else z_mid
        parts = len(scale_rows)
        for part, (scale, shift) in enumerate(scale_rows):
            ref = tile(k, s, c).at[part] if is_first(k) else tile(k, s, c)
            act = half_silu(ref[...].astype(F32) * scale + shift)
            if c in (0, cols + 1):
                act = jnp.where(has["left" if c == 0 else "right"], act, 0.0)
            at = cols - 1 + c
            above = jnp.concatenate([halo_act[0, part, at:at + 1, :], act[:-1]], axis=0)
            below = jnp.concatenate([act[1:], halo_act[1, part, at:at + 1, :]], axis=0)
            for dr, value in enumerate((above, act, below)):
                z[(c * 3 + dr) * parts + part] = value.astype(BF16)

    def wait_cols(k, s):
        for at, there in enumerate((has["right"], has["left"])):
            pl.when(there)(lambda at=at: col_copy(k, s, at).wait_recv())

    def layer(k, s):
        z = z_in if is_first(k) else z_mid
        scale_rows = scales(k, s)
        parts = len(scale_rows)
        depth = 3 * parts
        weights = (w_first[...] if is_first(k) else w_rest[number(k) - 1]).reshape(4 * depth * LANES, 2 * LANES)
        bias = bias_rows[number(k)]
        later = following(k)
        edge = edges(later, s)

        def pair(p, sums):
            acc = jnp.concatenate([jnp.dot(jnp.concatenate([z[2 * p * depth + i, lo:lo + rows // 2] for i in range(4 * depth)], axis=1), weights, preferred_element_type=F32)
                                   for lo in (0, rows // 2)], axis=0)
            sum_one, sum_two = sums
            for o in range(2):
                c = 2 * p + o
                value = acc[:, o * LANES:(o + 1) * LANES] + bias
                if k[1]:
                    value = value + short[s, c]
                rounded = value.astype(BF16)
                tile(later, s, c + 1)[...] = rounded
                value = rounded.astype(F32)
                if k[1]:
                    short[s, c] = value
                edge[0, 0, c:c + 1, :] = value[0:1]
                edge[1, 0, c:c + 1, :] = value[rows - 1:rows]
                value = value.reshape(rows // 8, 8, LANES)
                sum_one = sum_one + jnp.sum(value, axis=0)
                sum_two = sum_two + jnp.sum(value * value, axis=0)
            return sum_one, sum_two

        zero = jnp.zeros((8, LANES), F32)
        sums = (zero, zero)
        activate_rows(k, s, scale_rows)
        done = set()
        order = list(range(1, cols // 2 - 1)) + [0, cols // 2 - 1]
        for p in order:
            if p == 0 and is_first(k):
                for c in range(1, cols + 1):
                    if c not in done:
                        activate(k, s, scale_rows, c)
                        done.add(c)
                wait_cols(k, s)
            for c in range(2 * p, 2 * p + 4):
                if c not in done:
                    activate(k, s, scale_rows, c)
                    done.add(c)
            sums = pair(p, sums)
        target = message(later, s)
        for at, part in enumerate(sums):
            target[at:at + 1, :] = jnp.sum(part, axis=0, keepdims=True)
        send_stats(later, s)
        send_rows(later, s)
        send_cols(later, s)
        sent(k, s, first=True if is_first(k) else None)

    chunk = 16

    def load(s):
        pltpu.make_async_copy(act_hbm.at[s], raw.at[s], act_sem.at[s]).wait()

        def step(i, sums):
            at = pl.multiple_of(i * chunk, chunk)
            sums = list(sums)
            for part in range(halves):
                value = raw[s, pl.ds(at, chunk), :, part * LANES:(part + 1) * LANES].astype(F32)
                flat[s, part, pl.ds(pl.multiple_of(at * cols, chunk * cols), chunk * cols), :] = value.reshape(chunk * cols, LANES)
                sums[part] = sums[part] + jnp.sum(value, axis=0)
                sums[halves + part] = sums[halves + part] + jnp.sum(value * value, axis=0)
            return tuple(sums)

        zero = jnp.zeros((cols, LANES), F32)
        sums = lax.fori_loop(0, rows // chunk, step, (zero,) * (2 * halves))
        for at, part in enumerate(sums):
            msg_in[s, at:at + 1, :] = jnp.sum(part, axis=0, keepdims=True)
        for part in range(halves):
            edge_in[s, 0, part] = flat[s, part, 0:cols, :]
            edge_in[s, 1, part] = flat[s, part, (rows - 1) * cols:, :]

    def turn(s, c):
        for part in range(halves):
            map_in[s, c + 1, part] = flat[s, part, pl.ds(c, rows, stride=cols), :].astype(BF16)

    first = (0, 0)
    for s in range(samples):
        load(s)
    for s in range(samples):
        turn(s, 0)
        turn(s, cols - 1)
    pl.semaphore_wait(barrier, peers_n)
    send_stats(first, 0)
    for s in range(samples):
        send_rows(first, s)
        send_cols(first, s)

    for k in range(layers - 1):
        for o in range(2):
            for dc in range(3):
                pltpu.make_async_copy(w_rest_hbm.at[k, :, dc], w_rest.at[k, o + dc, :, :, pl.ds(o * LANES, LANES)], weight_sem.at[k + 1]).start()
    for src_dst, at in zip(small, range(len(small))):
        pltpu.make_async_copy(*src_dst, small_sem.at[at]).wait()
    row_id = lax.broadcasted_iota(jnp.int32, (LANES, LANES), 0)
    lane_id = lax.broadcasted_iota(jnp.int32, (LANES, LANES), 1)
    for ones, per_group in ((ones_in, in_ch // GROUPS), (ones_mid, LANES // GROUPS)):
        ones[...] = jnp.where(row_id // per_group == lane_id // per_group, 1.0, 0.0).astype(BF16)
    for dr in range(3):
        w_first[3, dr, :, 0:LANES] = jnp.zeros((in_ch, LANES), BF16)
        w_first[0, dr, :, LANES:] = jnp.zeros((in_ch, LANES), BF16)
    pltpu.make_async_copy(w_short_hbm, w_short, weight_sem.at[layers]).wait()
    for at in range(layers + 1):
        bias_rows[at] = bias_ref[at:at + 1].astype(F32)
    skip_bias = bias_rows[layers]
    def skip_product(s, _):
        for c in range(cols):
            if 0 < c < cols - 1:
                turn(s, c)
            both_halves = jnp.concatenate([map_in[s, c + 1, part] for part in range(halves)], axis=1)
            short[s, c] = jnp.dot(both_halves, w_short[...], preferred_element_type=F32) + skip_bias
        return 0

    lax.fori_loop(0, samples, skip_product, 0)

    def clear(k, _):
        for dr in range(3):
            w_rest[k, 3, dr, :, 0:LANES] = jnp.zeros((LANES, LANES), BF16)
            w_rest[k, 0, dr, :, LANES:] = jnp.zeros((LANES, LANES), BF16)
        return 0

    lax.fori_loop(0, layers - 1, clear, 0)

    col_id = lax.broadcasted_iota(jnp.int32, (cols, LANES), 0)

    def head_block(j, _):
        blocks = []
        for dr in range(3):
            for ch in range(3):
                block = jnp.zeros((cols, LANES), F32)
                for dc in range(3):
                    block = jnp.where(col_id == j - dc, w_out_ref[dr, dc, ch:ch + 1, :].astype(F32), block)
                blocks.append(block)
        blocks.append(jnp.zeros((cols, LANES), F32))
        w_head[:, pl.ds(pl.multiple_of(j * LANES, LANES), LANES)] = jnp.concatenate(blocks, axis=0).astype(BF16)
        return 0

    lax.fori_loop(0, cols + 2, head_block, 0)

    def both_samples(k):
        if not is_first(k):
            at = number(k) - 1
            pltpu.make_async_copy(w_rest.at[at, 0:3], w_rest.at[at, 0:3], weight_sem.at[at + 1]).wait()
        lax.fori_loop(0, samples, lambda s, _: (layer(k, s), 0)[1], 0)

    pltpu.make_async_copy(w_first.at[0:3], w_first.at[0:3], weight_sem.at[0]).wait()
    pltpu.make_async_copy(got_in, got_in, stat_recv.at[0, 0]).wait()
    both_samples(first)
    pltpu.make_async_copy(got_in, got_in, stat_send.at[0, 0]).wait()
    both_samples((0, 1))

    def block(i, _):
        both_samples((i, 0))
        both_samples((i, 1))
        return 0

    lax.fori_loop(1, layers // 2, block, 0)
    last = (layers // 2, 0)

    def head(s, _):
        scale_rows = scales(last, s)
        activate_rows(last, s, scale_rows)

        scale, shift = scale_rows[0]
        for c in range(cols + 2):
            act = half_silu(tile(last, s, c)[...].astype(F32) * scale + shift)
            if c in (0, cols + 1):
                act = jnp.where(has["left" if c == 0 else "right"], act, 0.0)
            z_mid[c] = act.astype(BF16)
            at = cols - 1 + c
            ends = [halo_act[side, 0, at:at + 1, :] for side in range(2)] + [jnp.zeros((14, LANES), F32)]
            z_edge[c] = jnp.concatenate(ends, axis=0).astype(BF16)

        def product(ref):
            acts = jnp.concatenate([ref[c] for c in range(cols + 2)], axis=1)
            return lax.dot_general(w_head[...], acts, (((1,), (1,)), ((), ())), preferred_element_type=F32)

        taps = product(z_mid)
        ends = product(z_edge)
        part = 3 * cols
        above = jnp.concatenate([ends[:part, 0:1], taps[:part, :-1]], axis=1)
        below = jnp.concatenate([taps[2 * part:3 * part, 1:], ends[2 * part:3 * part, 1:2]], axis=1)
        rgb = above + taps[part:2 * part] + below
        for ch in range(3):
            out_ref[s, ch] = rgb[ch * cols:(ch + 1) * cols] + bias_out_ref[:, ch:ch + 1].astype(F32)
        sent(last, s)
        return 0

    lax.fori_loop(0, samples, head, 0)


def solution(mesh):
    rows_n = mesh.shape["sy"]
    cols_n = mesh.shape["sx"]
    tile_spec = P("dp", "sy", "sx", None)
    replicated = P()

    def local_decode(act_in, norm_first, w_first, w_short, norm_rest, w_rest, bias_rest, w_out, bias_out):
        samples, rows, cols, in_ch = act_in.shape
        halves = in_ch // LANES
        layers = w_rest.shape[0] + 1
        peers_n = rows_n * cols_n - 1
        in_hbm = pl.BlockSpec(memory_space=pltpu.HBM)
        in_vmem = pl.BlockSpec(memory_space=pltpu.VMEM)
        image = pl.pallas_call(
            functools.partial(decode_kernel, rows_n, cols_n),
            out_shape=jax.ShapeDtypeStruct((samples, 3, cols, rows), F32),
            in_specs=[in_hbm] * 9,
            out_specs=in_vmem,
            scratch_shapes=[
                pltpu.VMEM((samples, rows, cols, in_ch), BF16),
                pltpu.VMEM((samples, halves, rows * cols, LANES), F32),
                pltpu.VMEM((samples, cols + 2, halves, rows, LANES), BF16),
                pltpu.VMEM(((layers + 1) // 2, samples, cols + 2, rows, LANES), BF16),
                pltpu.VMEM(((layers + 1) // 2, samples, cols + 2, rows, LANES), BF16),
                pltpu.VMEM(((cols + 2) * 3 * halves, rows, LANES), BF16),
                pltpu.VMEM(((cols + 2) * 3, rows, LANES), BF16),
                pltpu.VMEM((samples, cols, rows, LANES), F32),
                pltpu.VMEM((4, 3, in_ch, 2 * LANES), BF16),
                pltpu.VMEM((in_ch, LANES), BF16),
                pltpu.VMEM((layers - 1, 4, 3, LANES, 2 * LANES), BF16),
                pltpu.VMEM((10 * cols, (cols + 2) * LANES), BF16),
                pltpu.VMEM((cols + 2, 16, LANES), BF16),
                pltpu.VMEM((LANES, LANES), BF16),
                pltpu.VMEM((LANES, LANES), BF16),
                pltpu.VMEM(norm_first.shape, BF16),
                pltpu.VMEM(norm_rest.shape, BF16),
                pltpu.VMEM(bias_rest.shape, BF16),
                pltpu.VMEM((bias_rest.shape[0], 1, LANES), F32),
                pltpu.VMEM((3, 3, 3, LANES), BF16),
                pltpu.VMEM((1, 3), BF16),
                pltpu.VMEM((samples, 2 * halves, LANES), F32),
                pltpu.VMEM((layers, samples, 2, LANES), F32),
                pltpu.VMEM((peers_n, samples, 2 * halves, LANES), F32),
                pltpu.VMEM((layers, samples, peers_n, 2, LANES), F32),
                pltpu.VMEM((samples, 2, halves, cols, LANES), F32),
                pltpu.VMEM((layers, samples, 2, 1, cols, LANES), F32),
                pltpu.VMEM((samples, 2, 3, halves, cols, LANES), F32),
                pltpu.VMEM((layers, samples, 2, 3, 1, cols, LANES), F32),
                pltpu.VMEM((2, halves, 3 * cols, LANES), F32),
                pltpu.SemaphoreType.DMA((samples,)),
                pltpu.SemaphoreType.DMA((layers + 1,)),
                pltpu.SemaphoreType.DMA((5,)),
                pltpu.SemaphoreType.DMA((layers + 1, samples)),
                pltpu.SemaphoreType.DMA((layers + 1, samples)),
                pltpu.SemaphoreType.DMA((layers + 1, samples, 8)),
                pltpu.SemaphoreType.DMA((layers + 1, samples, 8)),
            ],
            compiler_params=pltpu.CompilerParams(collective_id=0, has_side_effects=True, vmem_limit_bytes=36 * 1024 * 1024),
            name="decode",
        )(*(pltpu.with_memory_space_constraint(x, pltpu.HBM) for x in (act_in, w_first, w_short, w_rest, norm_first, norm_rest, bias_rest, jnp.transpose(w_out, (0, 1, 3, 2)), bias_out.reshape(1, 3))))
        return jnp.transpose(image, (0, 3, 2, 1))

    return jax.shard_map(local_decode, mesh=mesh, in_specs=(tile_spec,) + (replicated,) * 8, out_specs=tile_spec, check_vma=False)
```
